32 devices in a mesh: wide: 16 (over z, x, core), lev: 2 (over y).
Axes of the slice: x: 2, y: 2, z: 4, core: 2. Of those that a mesh axis runs over, the one named last changes fastest.
Arguments:
- member_control: float32 [16, 16, 128], P('wide'), may hold values from -6 to 6
- static_control: float32 [8, 128, 1024], P('lev', 'wide'), may hold values from -6 to 6
- perturbations: bfloat16 [16, 8, 128, 1024], P(None, 'lev', 'wide'), may hold values from -6 to 6
- innovation: float32 [8, 128, 1024], P('lev', 'wide'), may hold values from -9 to 9
- diffusivity: float32 [8, 128, 1024], P('lev', 'wide'), may hold values from 0.05 to 0.15
- rows_factor: float32 [16, 16], replicated, may hold values from -1.5 to 1.5
- column_factor: float32 [128, 128], replicated, may hold values from -0.5 to 0.5
- ocean_mask: int32 [128, 1024], P('wide'), may hold values 0 or 1
- huber_blocks: int32 [8, 16, 128], P('lev', 'wide'), may hold values 0 or 1
- fold_map: int32 [1024], replicated, may hold values from 0 to 1023, as said below
Outputs:
- increment: float32 [8, 128, 1024], P('lev', 'wide')
- member_gradient: float32 [16, 16, 128], P('wide')
- static_gradient: float32 [8, 128, 1024], P('lev', 'wide')
The draws below stay inside these ranges and needn't reach their ends.
Inputs may be any that keep to these rules, and one draw needn't show every extreme that they name: fold_map[fold_map[j]] = j and fold_map[j] != j for every column j.
All inputs are finite; a program needn't handle non-finite values. No bound on the sum of `ocean_mask` or of `huber_blocks` on one device may be relied on, other than what follows from the above.
Results may differ from the reference program's by a relative error of at most 0.0003.
Values sent between devices are 32-bit elements; how exact they have to be, the bound alone decides.
No kernel may reach another device: no remote copies, remote signals or barrier semaphores. Data moves between devices by JAX's collectives and lax.ppermute only.
A program may use at most 64 MiB of HBM per device.

```python
import jax
import jax.numpy as jnp
from jax import lax

CW = 128
REFINE = 8
LEV = 8
STEPS = 3
MEMBERS = 16
CH = 16
FH = 128
FW = 1024


def draw_fold_map(key, part):
    shuffled = jax.random.permutation(jax.random.fold_in(key, 7), FW).astype(jnp.int32)
    first_half = shuffled[0::2]
    second = shuffled[1::2]
    partner = jnp.zeros((FW,), jnp.int32)
    partner = partner.at[first_half].set(second).at[second].set(first_half)
    return partner


def touch_ends(entries, key, low, largest):
    extent = entries.shape
    index_at = [jax.random.randint(jax.random.fold_in(key, axis), (), 0, extent[axis]) for axis in range(len(extent))]
    entries = entries.at[tuple(index_at)].set(low)
    longest = extent.index(max(extent))
    index_at[longest] = (index_at[longest] + 1) % extent[longest]
    return entries.at[tuple(index_at)].set(largest)


def levels(key, extent, cuts, smallest, largest):
    level, own = 1.0, jax.random.fold_in(key, 6)
    for axis_at, shards_of in cuts:
        steps = jnp.exp(jax.random.uniform(jax.random.fold_in(own, axis_at), (shards_of,), jnp.float32, smallest / len(cuts), largest / len(cuts)))
        level = level * jnp.repeat(steps, extent[axis_at] // shards_of).reshape([-1 if axis == axis_at else 1 for axis in range(len(extent))])
    return level


def scatter_about(stream_key, dims, spread, reach, shards=(), kind=jnp.bfloat16):
    level = levels(stream_key, dims, shards, -0.22, 0.18) if shards else 1.0
    entries = jax.random.normal(stream_key, dims, jnp.float32) * spread * level
    return jnp.minimum(jnp.maximum(entries, -reach), reach).astype(kind)


def setup_inputs(seed: int = 0) -> dict:
    keys = jax.random.split(jax.random.key(seed), 11)
    member_control = scatter_about(keys[0], (MEMBERS, CH, CW), 1.0, 6.0, ((0, 16),), jnp.float32)
    static_control = scatter_about(keys[1], (LEV, FH, FW), 1.0, 6.0, ((0, 2), (1, 16)), jnp.float32)
    perturbations = scatter_about(keys[2], (MEMBERS, LEV, FH, FW), 1.0, 6.0, ((1, 2), (2, 16)))
    innovation = scatter_about(keys[3], (LEV, FH, FW), 1.5, 9.0, ((0, 2), (1, 16)), jnp.float32)
    diffusivity = jnp.clip(0.05 + 0.10000001 * jax.random.uniform(keys[4], (LEV, FH, FW), jnp.float32) ** levels(keys[4], (LEV, FH, FW), ((0, 2), (1, 16)), -0.2, 0.2), 0.05, 0.15)
    rows_factor = scatter_about(keys[5], (CH, CH), CH ** -0.5, 1.5, (), jnp.float32)
    column_factor = scatter_about(keys[6], (CW, CW), CW ** -0.5, 0.5, (), jnp.float32)
    ocean_mask = touch_ends((jax.random.randint(keys[7], (FH, FW), 0, 5) < 4).astype(jnp.int32), jax.random.fold_in(keys[7], 1), 0, 1)
    huber_blocks = touch_ends((jax.random.randint(keys[8], (LEV, CH, CW), 0, 2) < 1).astype(jnp.int32), jax.random.fold_in(keys[8], 1), 0, 1)
    fold_map = draw_fold_map(jax.random.fold_in(keys[10], 71), 0)
    return dict(member_control=member_control, static_control=static_control, perturbations=perturbations, innovation=innovation, diffusivity=diffusivity, rows_factor=rows_factor, column_factor=column_factor, ocean_mask=ocean_mask, huber_blocks=huber_blocks, fold_map=fold_map)


HUBER_EDGE = 1.0
VERTICAL_WEIGHT = 0.5
PRECISE = lax.Precision.HIGHEST

def smooth_fields(values, rows_factor, column_factor):
    left_done = jnp.einsum('ij,mjk->mik', rows_factor, values, precision=PRECISE)
    return jnp.einsum('mik,kl->mil', left_done, column_factor, precision=PRECISE)

def smooth_adjoint(values, rows_factor, column_factor):
    left_done = jnp.einsum('ji,mjk->mik', rows_factor, values, precision=PRECISE)
    return jnp.einsum('mik,lk->mil', left_done, column_factor, precision=PRECISE)

def interpolate(extended, refine):
    fraction = jnp.arange(refine, dtype=jnp.float32) / refine
    below_row = extended[..., :-1, None, :]
    above_row = extended[..., 1:, None, :]
    row_terms = below_row * (1.0 - fraction)[:, None] + above_row * fraction[:, None]
    dims_of = row_terms.shape
    row_terms = row_terms.reshape(dims_of[:-3] + (dims_of[-3] * refine, dims_of[-1]))
    wrapped = jnp.roll(row_terms, -1, axis=-1)
    col_terms = row_terms[..., None] * (1.0 - fraction) + wrapped[..., None] * fraction
    return col_terms.reshape(row_terms.shape[:-1] + (row_terms.shape[-1] * refine,))

def interpolate_adjoint(fine_field, refine):
    fraction = jnp.arange(refine, dtype=jnp.float32) / refine
    dims_of = fine_field.shape
    col_terms = fine_field.reshape(dims_of[:-1] + (dims_of[-1] // refine, refine))
    coarse_cols = lax.optimization_barrier(jnp.sum(col_terms * (1.0 - fraction), axis=-1)) + jnp.roll(lax.optimization_barrier(jnp.sum(col_terms * fraction, axis=-1)), 1, axis=-1)
    row_terms = coarse_cols.reshape(dims_of[:-2] + (dims_of[-2] // refine, refine, dims_of[-1] // refine))
    below_part = lax.optimization_barrier(jnp.sum(row_terms * (1.0 - fraction)[:, None], axis=-2))
    above_part = lax.optimization_barrier(jnp.sum(row_terms * fraction[:, None], axis=-2))
    zero_row = jnp.zeros_like(below_part[..., :1, :])
    return jnp.concatenate([below_part, zero_row], axis=-2) + jnp.concatenate([zero_row, above_part], axis=-2)

def diffuse(values, diffusivity, fold_map):
    root_kappa = jnp.sqrt(diffusivity)
    for _ in range(STEPS):
        scaled = root_kappa * values
        padded = jnp.pad(scaled, ((1, 1), (1, 1), (0, 0)))
        folded = jnp.take(scaled[:, -1, :], fold_map, axis=1)
        padded = padded.at[1:-1, -1, :].set(folded)
        across = padded[1:-1, 2:, :] + padded[1:-1, :-2, :] + jnp.roll(scaled, 1, axis=2) + jnp.roll(scaled, -1, axis=2) - 4.0 * scaled
        vertical = padded[2:, 1:-1, :] + padded[:-2, 1:-1, :] - 2.0 * scaled
        values = values + root_kappa * (across + VERTICAL_WEIGHT * vertical)
    return values

def huber_weigh(increment, innovation, ocean_cells, huber_blocks):
    misfit = increment - innovation
    expanded = jnp.repeat(jnp.repeat(huber_blocks, REFINE, axis=1), REFINE, axis=2)
    weight = jnp.where(expanded == 1, HUBER_EDGE / jnp.maximum(jnp.abs(misfit), HUBER_EDGE), 1.0)
    return ocean_cells * weight * misfit

def reference(member_control, static_control, perturbations, innovation, diffusivity, rows_factor, column_factor, ocean_mask, huber_blocks, fold_map):
    member_scale = (MEMBERS - 1) ** (-0.5)
    smoothed = smooth_fields(member_control, rows_factor, column_factor)
    extended = jnp.concatenate([smoothed, smoothed[:, -1:, :]], axis=1)

    def add_member(running, member_pair):
        ext_one, pert_one = member_pair
        fine_field = interpolate(ext_one, REFINE)
        return (running + fine_field[None] * pert_one, None)
    initial = jnp.zeros((LEV, FH, FW), jnp.float32)
    ensemble, _ = lax.scan(add_member, initial, (extended, perturbations))
    ocean_cells = ocean_mask.astype(jnp.float32)
    increment = ocean_cells * (member_scale * ensemble + diffuse(static_control, diffusivity, fold_map))
    weighted = huber_weigh(increment, innovation, ocean_cells, huber_blocks)
    static_gradient = static_control + diffuse(weighted, diffusivity, fold_map)

    def member_terms(pert_one):
        fine_terms = lax.optimization_barrier(jnp.sum(pert_one * weighted, axis=0)) * member_scale
        return interpolate_adjoint(fine_terms, REFINE)
    ext_grad = lax.map(member_terms, perturbations)
    smooth_grad = ext_grad[:, :-1, :].at[:, -1, :].add(ext_grad[:, -1, :])
    member_gradient = member_control + smooth_adjoint(smooth_grad, rows_factor, column_factor)
    return (increment, member_gradient, static_gradient)
```

```python
import functools

import jax
import jax.numpy as jnp
from jax import lax
from jax.experimental import pallas as pl
from jax.experimental.pallas import tpu as pltpu
from jax.sharding import PartitionSpec as P

STEPS = 3
HUBER_EDGE = 1.0
VERTICAL_WEIGHT = 0.5
PRECISE = lax.Precision.HIGHEST
LANES = 128
GROUP = 16
F32 = jnp.float32
BF16 = jnp.bfloat16


def dot_precise(left, right, dims=((1,), (0,))):
    return lax.dot_general(left, right, (dims, ((), ())), precision=PRECISE, preferred_element_type=F32)


def dot_split(left, right, dims=((1,), (0,))):
    high = left.astype(BF16)
    rest = left - high.astype(F32)
    middle = rest.astype(BF16)
    low = (rest - middle.astype(F32)).astype(BF16)
    parts = [
        lax.dot_general(part, right, (dims, ((), ())), preferred_element_type=F32)
        for part in (low, middle, high)
    ]
    return (parts[0] + parts[1]) + parts[2]


def iota(shape, dim):
    return lax.broadcasted_iota(jnp.int32, shape, dim)


def level_at(entry, levels, lev):
    return jnp.where(lev == 0, entry, levels - 1 - entry)


def row_plan(levels, with_kappa):
    plan = [(False, d, e) for d in range(1, STEPS + 1) for e in range(levels + STEPS - d)]
    if with_kappa:
        plan += [(True, d, e) for d in range(1, STEPS) for e in range(levels + STEPS - 1 - d)]
    return plan


def padded_rows(levels, with_kappa):
    return -(-len(row_plan(levels, with_kappa)) // 8) * 8


def start_kernel(value, kappa, member, rows_f, cols_f, swap, windows):
    levels, rows, _ = value.shape
    lev = lax.axis_index("lev")
    for j in range(STEPS):
        at = level_at(levels - 1 - j, levels, lev)
        k = kappa[at]
        swap[j * rows : (j + 1) * rows, :] = jnp.sqrt(k) * value[at]
        if j < STEPS - 1:
            swap[(STEPS + j) * rows : (STEPS + j + 1) * rows, :] = k
    coarse = rows_f.shape[0]
    shape = (2 * coarse, coarse)
    pair = iota(shape, 0)
    wanted = jnp.minimum(pair // 2 + pair % 2, coarse - 1)
    pick = jnp.where(iota(shape, 1) == wanted, 1.0, 0.0).astype(F32)
    right_done = dot_precise(member[0], cols_f[...])
    windows[...] = dot_precise(dot_precise(pick, rows_f[...]), right_done)


def pack_rows(plan, row_of, up, down, rows):
    for j, (is_kappa, d, e) in enumerate(plan):
        up[j : j + 1, :] = row_of(is_kappa, e, rows - d)
        down[j : j + 1, :] = row_of(is_kappa, e, d - 1)
    for j in range(len(plan), up.shape[0]):
        up[j : j + 1, :] = jnp.zeros((1, up.shape[1]), F32)
        down[j : j + 1, :] = jnp.zeros((1, up.shape[1]), F32)


def pack_static_kernel(value, kappa, swap, blocks, up, down, interp, huber):
    levels, rows, width = value.shape
    lev = lax.axis_index("lev")

    def row_of(is_kappa, e, r):
        if e >= levels:
            start = (e - levels + (STEPS if is_kappa else 0)) * rows
            return swap[start + r : start + r + 1, :]
        at = level_at(e, levels, lev)
        k = kappa[at, r : r + 1, :]
        return k if is_kappa else jnp.sqrt(k) * value[at, r : r + 1, :]

    pack_rows(row_plan(levels, True), row_of, up, down, rows)
    coarse = interp.shape[0]
    refine = width // coarse
    shape = (coarse, width)
    column = iota(shape, 1)
    at = iota(shape, 0)
    cell = column // refine
    fraction = (column % refine).astype(F32) * (1.0 / refine)
    following = jnp.where(cell == coarse - 1, 0, cell + 1)
    below = cell == at
    interp[...] = (
        jnp.where(below, 1.0 - fraction, 0.0) + jnp.where(following == at, fraction, 0.0)
    ).astype(BF16)
    spread = jnp.where(below, 1.0, 0.0).astype(BF16)
    huber[...] = jnp.dot(blocks[...].astype(F32).astype(BF16), spread, preferred_element_type=F32)


def pack_weighted_kernel(scaled, swap, up, down):
    levels, rows, _ = scaled.shape

    def row_of(is_kappa, e, r):
        if e >= levels:
            start = (e - levels) * rows
            return swap[start + r : start + r + 1, :]
        return scaled[e, r : r + 1, :]

    pack_rows(row_plan(levels, False), row_of, up, down, rows)


def unpack_rows(plan, state, kappa_ext, low, high, rows):
    is_first = lax.axis_index("wide") == 0
    for j, (is_kappa, d, e) in enumerate(plan):
        target = kappa_ext if is_kappa else state
        before = low[j : j + 1, :]
        target[e, 2 * rows - d : 2 * rows - d + 1, :] = jnp.where(is_first, 0.0, before)
        target[e, rows + d - 1 : rows + d, :] = high[j : j + 1, :]


def diffuse_steps(state, kappa_ext, total, fold, edge, levels, rows, width, finish):
    is_last = lax.axis_index("wide") == lax.axis_size("wide") - 1
    tiles = width // LANES
    for step in range(STEPS):
        updated = levels + STEPS - 1 - step

        @pl.when(is_last)
        def _():
            for e in range(updated):
                edge[e : e + 1, :] = state[e, rows - 1 : rows, :]
            for t in range(tiles):
                index = jnp.broadcast_to(fold[:, t * LANES : (t + 1) * LANES], (8, LANES))
                lane = lax.rem(index, LANES)
                source = lax.div(index, LANES)
                found = jnp.zeros((8, LANES), F32)
                for q in range(tiles):
                    part = jnp.take_along_axis(
                        edge[:, q * LANES : (q + 1) * LANES], lane, axis=1, mode="promise_in_bounds"
                    )
                    found = jnp.where(source == q, part, found)
                for e in range(updated):
                    state[e, rows : rows + 1, t * LANES : (t + 1) * LANES] = found[e : e + 1, :]

        below = None
        for e in range(updated):
            whole = state[e]
            with_halo = step < STEPS - 1 and e < updated - 1
            kept = 2 * rows if with_halo else rows
            here = whole[:kept]
            above = state[e + 1, :kept, :]
            vertical = above if below is None else above + below[:kept]
            across = (
                pltpu.roll(whole, 2 * rows - 1, 0)[:kept]
                + pltpu.roll(whole, 1, 0)[:kept]
                + pltpu.roll(here, width - 1, 1)
                + pltpu.roll(here, 1, 1)
            )
            change = across + VERTICAL_WEIGHT * vertical - (4.0 + 2.0 * VERTICAL_WEIGHT) * here
            below = whole
            if step < STEPS - 1:
                state[e, :kept, :] = here + kappa_ext[e, :kept, :] * change
            if e < levels:
                if step == 0:
                    total[e] = change[:rows]
                elif step < STEPS - 1:
                    total[e] = total[e] + change[:rows]
                else:
                    finish(e, total[e] + change[:rows])


def static_kernel(value, kappa, swap, low, high, fold, diffused, kappa_ext, state, total, edge):
    levels, rows, width = value.shape
    lev = lax.axis_index("lev")
    zero = jnp.zeros((rows, width), F32)
    edge[...] = jnp.zeros(edge.shape, F32)
    for e in range(levels + STEPS):
        state[e, rows:, :] = zero
        if e < levels + STEPS - 1:
            kappa_ext[e, rows:, :] = zero
        if e < levels:
            at = level_at(e, levels, lev)
            k = kappa[at]
            kappa_ext[e, :rows, :] = k
            state[e, :rows, :] = jnp.sqrt(k) * value[at]
        else:
            start = (e - levels) * rows
            state[e, :rows, :] = swap[start : start + rows, :]
            if e < levels + STEPS - 1:
                start += STEPS * rows
                kappa_ext[e, :rows, :] = swap[start : start + rows, :]
    unpack_rows(row_plan(levels, True), state, kappa_ext, low, high, rows)

    def finish(e, change):
        at = level_at(e, levels, lev)
        diffused[at] = value[at] + jnp.sqrt(kappa[at]) * change

    diffuse_steps(state, kappa_ext, total, fold, edge, levels, rows, width, finish)


def weighted_kernel(
    value, weighted, kappa, kappa_ext, scaled, swap, low, high, fold, gradient, state, ring, total, edge
):
    levels, rows, width = value.shape
    lev = lax.axis_index("lev")
    zero = jnp.zeros((rows, width), F32)
    edge[...] = jnp.zeros(edge.shape, F32)
    for e in range(levels + STEPS):
        state[e, rows:, :] = zero
        if e < levels:
            state[e, :rows, :] = scaled[e]
        else:
            start = (e - levels) * rows
            state[e, :rows, :] = swap[start : start + rows, :]
    unpack_rows(row_plan(levels, False), state, ring, low, high, rows)

    def finish(e, change):
        at = level_at(e, levels, lev)
        gradient[at] = value[at] + (weighted[at] + jnp.sqrt(kappa[at]) * change)

    diffuse_steps(state, kappa_ext, total, fold, edge, levels, rows, width, finish)


def ensemble_kernel(
    windows, interp, perturbations, diffused, innovation, kappa, mask, huber, increment, weighted, scaled, swap, coarse
):
    members, levels, rows, width = perturbations.shape
    lev = lax.axis_index("lev")
    coarse[...] = dot_split(windows[...], interp[...])
    fraction = iota((rows, width), 0).astype(F32) * (1.0 / rows)

    def add_group(first, sums):
        sums = list(sums)
        for m in range(min(GROUP, members)):
            at = first + m
            fine = (1.0 - fraction) * coarse[pl.ds(2 * at, 1), :] + fraction * coarse[pl.ds(2 * at + 1, 1), :]
            for l in range(levels):
                sums[l] = sums[l] + fine * perturbations[at, l].astype(F32)
        return tuple(sums)

    sums = tuple(jnp.zeros((rows, width), F32) for _ in range(levels))
    if members <= GROUP:
        sums = add_group(0, sums)
    else:
        sums = lax.fori_loop(0, members // GROUP, lambda g, s: add_group(g * GROUP, s), sums)
    ocean = mask[...].astype(F32)
    scale = (members - 1) ** (-0.5)
    for l in range(levels):
        grown = ocean * (scale * sums[l] + diffused[l])
        increment[l] = grown
        misfit = grown - innovation[l]
        weight = jnp.where(
            huber[l : l + 1, :] > 0.5, HUBER_EDGE / jnp.maximum(jnp.abs(misfit), HUBER_EDGE), 1.0
        )
        kept = ocean * weight * misfit
        weighted[l] = kept
        rooted = jnp.sqrt(kappa[l]) * kept
        entry = level_at(l, levels, lev)
        scaled[entry] = rooted

        @pl.when(entry > 0)
        def _():
            swap[pl.ds(pl.multiple_of((levels - 1 - entry) * rows, 8), rows), :] = rooted


def terms_kernel(perturbations, weighted, interp, sent, terms):
    members, levels, rows, width = perturbations.shape
    group = min(GROUP, members)
    scale = (members - 1) ** (-0.5)
    shape = (4 * group, group * rows)
    pair = iota(shape, 0)
    column = iota(shape, 1)
    fraction = (column % rows).astype(F32) * (1.0 / rows)
    share = jnp.where(pair % 2 == 0, 1.0 - fraction, fraction)
    share = jnp.where(column // rows == pair // 4, share, 0.0)
    held = [weighted[l] for l in range(levels)]

    def one_group(first):
        for m in range(group):
            term = held[0] * perturbations[first + m, 0].astype(F32)
            for l in range(1, levels):
                term = term + held[l] * perturbations[first + m, l].astype(F32)
            terms[m * rows : (m + 1) * rows, :] = term
        narrow = dot_split(terms[...], interp[...], ((1,), (1,)))
        sent[pl.ds(pl.multiple_of(4 * first, 8), 4 * group), :] = scale * dot_precise(share, narrow)

    if members <= GROUP:
        one_group(0)
    else:
        lax.fori_loop(0, members // GROUP, lambda g, c: (one_group(g * GROUP), c)[1], 0)


def member_kernel(received, member, rows_f, cols_f, gradient):
    coarse = rows_f.shape[0]
    shape = (coarse, received.shape[0])
    source = iota(shape, 1)
    wanted = jnp.minimum(source // 4 + source % 2, coarse - 1)
    gather = jnp.where(iota(shape, 0) == wanted, 1.0, 0.0).astype(F32)
    smooth = dot_precise(gather, received[...])
    right_done = dot_precise(smooth, cols_f[...], ((1,), (1,)))
    gradient[0] = member[0] + dot_precise(rows_f[...], right_done, ((0,), (0,)))


def call(kernel, outs, scratch=(), name=None, flops=100000):
    return pl.pallas_call(
        kernel,
        out_shape=[jax.ShapeDtypeStruct(shape, dtype) for shape, dtype in outs],
        scratch_shapes=[pltpu.VMEM(shape, dtype) for shape, dtype in scratch],
        cost_estimate=pl.CostEstimate(flops=flops, transcendentals=0, bytes_accessed=0),
        name=name,
    )


def on_device(
    member_control,
    static_control,
    perturbations,
    innovation,
    diffusivity,
    rows_factor,
    column_factor,
    ocean_mask,
    huber_blocks,
    fold_map,
):
    members, levels, rows, width = perturbations.shape
    wide, lev = lax.axis_size("wide"), lax.axis_size("lev")
    coarse_rows, coarse = rows_factor.shape[0], column_factor.shape[0]
    assert lev == 2 and members == wide and coarse_rows == wide and rows == 8 and levels >= STEPS
    ring_up = [(i, (i + 1) % wide) for i in range(wide)]
    ring_down = [(j, i) for i, j in ring_up]
    partner = [(0, 1), (1, 0)]
    cell = (levels, rows, width)
    fold = fold_map.reshape(1, width)
    blocks = huber_blocks.reshape(levels, coarse)

    swap, windows = call(
        start_kernel,
        [(((2 * STEPS - 1) * rows, width), F32), ((2 * coarse_rows, coarse), F32)],
        name="start",
    )(static_control, diffusivity, member_control, rows_factor, column_factor)
    swap = lax.ppermute(swap, "lev", partner)
    windows = lax.all_to_all(windows.reshape(wide, 2, coarse), "wide", 0, 0, tiled=True)
    windows = windows.reshape(2 * members, coarse)
    count = padded_rows(levels, True)
    up, down, interp, huber = call(
        pack_static_kernel,
        [((count, width), F32), ((count, width), F32), ((coarse, width), BF16), ((levels, width), F32)],
        name="pack_static",
    )(static_control, diffusivity, swap, blocks)
    low = lax.ppermute(up, "wide", ring_up)
    high = lax.ppermute(down, "wide", ring_down)
    entries = levels + STEPS
    diffused, kappa_ext = call(
        static_kernel,
        [(cell, F32), ((entries - 1, 2 * rows, width), F32)],
        [((entries, 2 * rows, width), F32), (cell, F32), ((8, width), F32)],
        name="diffuse_static",
    )(static_control, diffusivity, swap, low, high, fold)
    increment, weighted, scaled, swap = call(
        ensemble_kernel,
        [(cell, F32), (cell, F32), (cell, F32), ((STEPS * rows, width), F32)],
        [((2 * members, width), F32)],
        name="ensemble",
    )(windows, interp, perturbations, diffused, innovation, diffusivity, ocean_mask, huber)
    swap = lax.ppermute(swap, "lev", partner)
    (sent,) = call(
        terms_kernel,
        [((4 * members, coarse), F32)],
        [((min(GROUP, members) * rows, width), F32)],
        name="terms",
    )(perturbations, weighted, interp)
    received = lax.all_to_all(
        sent.reshape(2 * members, 2, coarse), ("wide", "lev"), 0, 0, tiled=True
    ).reshape(4 * members, coarse)
    count = padded_rows(levels, False)
    up, down = call(
        pack_weighted_kernel,
        [((count, width), F32), ((count, width), F32)],
        name="pack_weighted",
    )(scaled, swap)
    low = lax.ppermute(up, "wide", ring_up)
    high = lax.ppermute(down, "wide", ring_down)
    (static_gradient,) = call(
        weighted_kernel,
        [(cell, F32)],
        [((entries, 2 * rows, width), F32), ((8, LANES), F32), (cell, F32), ((8, width), F32)],
        name="diffuse_weighted",
    )(static_control, weighted, diffusivity, kappa_ext, scaled, swap, low, high, fold)
    (member_gradient,) = call(member_kernel, [(member_control.shape, F32)], name="member")(
        received, member_control, rows_factor, column_factor
    )
    return (increment, member_gradient, static_gradient)


def solution(mesh):
    return jax.shard_map(
        on_device,
        mesh=mesh,
        in_specs=(
            P("wide", None, None),
            P("lev", "wide", None),
            P(None, "lev", "wide", None),
            P("lev", "wide", None),
            P("lev", "wide", None),
            P(),
            P(),
            P("wide", None),
            P("lev", "wide", None),
            P(),
        ),
        out_specs=(P("lev", "wide", None), P("wide", None, None), P("lev", "wide", None)),
        check_vma=False,
    )
```

```python
import jax
import jax.numpy as jnp
from jax import lax
from jax.experimental import pallas as pl
from jax.experimental.pallas import tpu as pltpu
from jax.sharding import PartitionSpec as P


STEPS = 3
HUBER_EDGE = 1.0
VERTICAL_WEIGHT = 0.5
PRECISE = lax.Precision.HIGHEST
LANES = 128
GROUP = 16
VMEM_BYTES = 32 * 2**20
F32 = jnp.float32
BF16 = jnp.bfloat16


def dot_precise(left, right, dims=((1,), (0,))):
    return lax.dot_general(left, right, (dims, ((), ())), precision=PRECISE, preferred_element_type=F32)


def sum_parts(array, product):
    high = array.astype(BF16)
    rest = array - high.astype(F32)
    middle = rest.astype(BF16)
    low = (rest - middle.astype(F32)).astype(BF16)
    return (product(low) + product(middle)) + product(high)


def dot_split(left, right, dims=((1,), (0,))):
    return sum_parts(left, lambda part: lax.dot_general(part, right, (dims, ((), ())), preferred_element_type=F32))


def iota(shape, dim):
    return lax.broadcasted_iota(jnp.int32, shape, dim)


def level_at(entry, levels, lev):
    return jnp.where(lev == 0, entry, levels - 1 - entry)


def row_plan(levels, with_kappa):
    plan = [(False, d, e) for d in range(1, STEPS + 1) for e in range(levels + STEPS - d)]
    if with_kappa:
        plan += [(True, d, e) for d in range(1, STEPS) for e in range(levels + STEPS - 1 - d)]
    return plan


def padded_rows(levels, with_kappa):
    return -(-len(row_plan(levels, with_kappa)) // 8) * 8


def start_kernel(
    value_h, kappa_h, member_h, rows_h, cols_h, blocks_h, fold_h, swap, windows, value, kappa, member, rows_f, cols_f, blocks, fold, done
):
    levels, rows, _ = value.shape
    coarse = rows_f.shape[0]
    lev = lax.axis_index("lev")
    sources = (member_h, cols_h, rows_h, kappa_h, value_h, blocks_h, fold_h)
    targets = (member, cols_f, rows_f, kappa, value, blocks, fold)
    copies = [pltpu.make_async_copy(s, t, done.at[i]) for i, (s, t) in enumerate(zip(sources, targets))]
    for copy in copies:
        copy.start()
    for copy in copies[:3]:
        copy.wait()
    smoothed = dot_precise(rows_f[...], dot_precise(member[0], cols_f[...]))
    windows[pl.ds(0, coarse, stride=2), :] = smoothed
    ring = pltpu.roll(smoothed, coarse - 1, 0)
    windows[pl.ds(1, coarse, stride=2), :] = jnp.where(iota(smoothed.shape, 0) == coarse - 1, smoothed, ring)
    for copy in copies[3:]:
        copy.wait()
    for j in range(STEPS):
        at = level_at(levels - 1 - j, levels, lev)
        k = kappa[at]
        swap[j * rows : (j + 1) * rows, :] = jnp.sqrt(k) * value[at]
        if j < STEPS - 1:
            swap[(STEPS + j) * rows : (STEPS + j + 1) * rows, :] = k


def pack_rows(plan, row_of, up, down, rows):
    for j, (is_kappa, d, e) in enumerate(plan):
        up[j : j + 1, :] = row_of(is_kappa, e, rows - d)
        down[j : j + 1, :] = row_of(is_kappa, e, d - 1)
    for j in range(len(plan), up.shape[0]):
        up[j : j + 1, :] = jnp.zeros((1, up.shape[1]), F32)
        down[j : j + 1, :] = jnp.zeros((1, up.shape[1]), F32)


def pack_static_kernel(value, kappa, swap, blocks, up, down, interp, huber):
    levels, rows, width = value.shape
    lev = lax.axis_index("lev")

    def row_of(is_kappa, e, r):
        if e >= levels:
            start = (e - levels + (STEPS if is_kappa else 0)) * rows
            return swap[start + r : start + r + 1, :]
        at = level_at(e, levels, lev)
        k = kappa[at, r : r + 1, :]
        return k if is_kappa else jnp.sqrt(k) * value[at, r : r + 1, :]

    pack_rows(row_plan(levels, True), row_of, up, down, rows)
    coarse = interp.shape[0]
    refine = width // coarse
    shape = (coarse, width)
    column = iota(shape, 1)
    at = iota(shape, 0)
    cell = column // refine
    fraction = (column % refine).astype(F32) * (1.0 / refine)
    following = jnp.where(cell == coarse - 1, 0, cell + 1)
    below = cell == at
    interp[...] = (
        jnp.where(below, 1.0 - fraction, 0.0) + jnp.where(following == at, fraction, 0.0)
    ).astype(BF16)
    spread = jnp.where(below, 1.0, 0.0).astype(BF16)
    huber[...] = jnp.dot(blocks[...].astype(F32).astype(BF16), spread, preferred_element_type=F32)


def pack_weighted_kernel(scaled, swap, up, down):
    levels, rows, _ = scaled.shape

    def row_of(is_kappa, e, r):
        if e >= levels:
            start = (e - levels) * rows
            return swap[start + r : start + r + 1, :]
        return scaled[e, r : r + 1, :]

    pack_rows(row_plan(levels, False), row_of, up, down, rows)


def unpack_rows(plan, state, kappa_ext, low, high, rows):
    is_first = lax.axis_index("wide") == 0
    for j, (is_kappa, d, e) in enumerate(plan):
        target = kappa_ext if is_kappa else state
        before = low[j : j + 1, :]
        target[e, 2 * rows - d : 2 * rows - d + 1, :] = jnp.where(is_first, 0.0, before)
        target[e, rows + d - 1 : rows + d, :] = high[j : j + 1, :]


def diffuse_steps(state, kappa_ext, total, fold, edge, levels, rows, width, finish):
    is_last = lax.axis_index("wide") == lax.axis_size("wide") - 1
    tiles = width // LANES
    for step in range(STEPS):
        updated = levels + STEPS - 1 - step

        @pl.when(is_last)
        def _():
            for e in range(updated):
                edge[e : e + 1, :] = state[e, rows - 1 : rows, :]
            for t in range(tiles):
                index = jnp.broadcast_to(fold[:, t * LANES : (t + 1) * LANES], (8, LANES))
                lane = lax.rem(index, LANES)
                source = lax.div(index, LANES)
                found = jnp.zeros((8, LANES), F32)
                for q in range(tiles):
                    part = jnp.take_along_axis(
                        edge[:, q * LANES : (q + 1) * LANES], lane, axis=1, mode="promise_in_bounds"
                    )
                    found = jnp.where(source == q, part, found)
                for e in range(updated):
                    state[e, rows : rows + 1, t * LANES : (t + 1) * LANES] = found[e : e + 1, :]

        below = None
        for e in range(updated):
            whole = state[e]
            with_halo = step < STEPS - 1 and e < updated - 1
            kept = 2 * rows if with_halo else rows
            here = whole[:kept]
            above = state[e + 1, :kept, :]
            vertical = above if below is None else above + below[:kept]
            across = (
                pltpu.roll(whole, 2 * rows - 1, 0)[:kept]
                + pltpu.roll(whole, 1, 0)[:kept]
                + pltpu.roll(here, width - 1, 1)
                + pltpu.roll(here, 1, 1)
            )
            change = across + VERTICAL_WEIGHT * vertical - (4.0 + 2.0 * VERTICAL_WEIGHT) * here
            below = whole
            if step < STEPS - 1:
                state[e, :kept, :] = here + kappa_ext[e, :kept, :] * change
            if e < levels:
                if step == 0:
                    total[e] = change[:rows]
                elif step < STEPS - 1:
                    total[e] = total[e] + change[:rows]
                else:
                    finish(e, total[e] + change[:rows])


def static_kernel(value, kappa, swap, low, high, fold, diffused, kappa_ext, state, total, edge):
    levels, rows, width = value.shape
    lev = lax.axis_index("lev")
    zero = jnp.zeros((rows, width), F32)
    edge[...] = jnp.zeros(edge.shape, F32)
    for e in range(levels + STEPS):
        state[e, rows:, :] = zero
        if e < levels + STEPS - 1:
            kappa_ext[e, rows:, :] = zero
        if e < levels:
            at = level_at(e, levels, lev)
            k = kappa[at]
            kappa_ext[e, :rows, :] = k
            state[e, :rows, :] = jnp.sqrt(k) * value[at]
        else:
            start = (e - levels) * rows
            state[e, :rows, :] = swap[start : start + rows, :]
            if e < levels + STEPS - 1:
                start += STEPS * rows
                kappa_ext[e, :rows, :] = swap[start : start + rows, :]
    unpack_rows(row_plan(levels, True), state, kappa_ext, low, high, rows)

    def finish(e, change):
        at = level_at(e, levels, lev)
        diffused[at] = value[at] + jnp.sqrt(kappa[at]) * change

    diffuse_steps(state, kappa_ext, total, fold, edge, levels, rows, width, finish)


def weighted_kernel(
    value, weighted, kappa, kappa_ext, scaled, swap, low, high, fold, gradient, state, ring, total, edge
):
    levels, rows, width = value.shape
    lev = lax.axis_index("lev")
    zero = jnp.zeros((rows, width), F32)
    edge[...] = jnp.zeros(edge.shape, F32)
    for e in range(levels + STEPS):
        state[e, rows:, :] = zero
        if e < levels:
            state[e, :rows, :] = scaled[e]
        else:
            start = (e - levels) * rows
            state[e, :rows, :] = swap[start : start + rows, :]
    unpack_rows(row_plan(levels, False), state, ring, low, high, rows)

    def finish(e, change):
        at = level_at(e, levels, lev)
        gradient[at] = value[at] + (weighted[at] + jnp.sqrt(kappa[at]) * change)

    diffuse_steps(state, kappa_ext, total, fold, edge, levels, rows, width, finish)


def ensemble_kernel(
    windows, interp, perturbations, diffused, innovation, kappa, mask, huber, increment, weighted, scaled, swap, coarse
):
    members, levels, rows, width = perturbations.shape
    lev = lax.axis_index("lev")
    coarse[...] = dot_split(windows[...], interp[...])
    fraction = iota((rows, width), 0).astype(F32) * (1.0 / rows)

    def add_group(first, sums):
        sums = list(sums)
        for m in range(min(GROUP, members)):
            at = first + m
            fine = (1.0 - fraction) * coarse[pl.ds(2 * at, 1), :] + fraction * coarse[pl.ds(2 * at + 1, 1), :]
            for l in range(levels):
                sums[l] = sums[l] + fine * perturbations[at, l].astype(F32)
        return tuple(sums)

    sums = tuple(jnp.zeros((rows, width), F32) for _ in range(levels))
    if members <= GROUP:
        sums = add_group(0, sums)
    else:
        sums = lax.fori_loop(0, members // GROUP, lambda g, s: add_group(g * GROUP, s), sums)
    ocean = mask[...].astype(F32)
    scale = (members - 1) ** (-0.5)
    for l in range(levels):
        grown = ocean * (scale * sums[l] + diffused[l])
        increment[l] = grown
        misfit = grown - innovation[l]
        weight = jnp.where(
            huber[l : l + 1, :] > 0.5, HUBER_EDGE / jnp.maximum(jnp.abs(misfit), HUBER_EDGE), 1.0
        )
        kept = ocean * weight * misfit
        weighted[l] = kept
        rooted = jnp.sqrt(kappa[l]) * kept
        entry = level_at(l, levels, lev)
        scaled[entry] = rooted

        @pl.when(entry > 0)
        def _():
            swap[pl.ds(pl.multiple_of((levels - 1 - entry) * rows, 8), rows), :] = rooted


def terms_kernel(perturbations, weighted, interp, sent, terms):
    members, levels, rows, _ = perturbations.shape
    group = min(GROUP, members)
    scale = (members - 1) ** (-0.5)
    shape = (4 * group, group * rows)
    pair = iota(shape, 0)
    column = iota(shape, 1)
    fraction = (column % rows).astype(F32) * (1.0 / rows)
    share = jnp.where(pair % 2 == 0, 1.0 - fraction, fraction)
    share = jnp.where(column // rows == pair // 4, share, 0.0).astype(BF16)
    held = [weighted[l] for l in range(levels)]

    def one_group(first):
        for m in range(group):
            term = held[0] * perturbations[first + m, 0].astype(F32)
            for l in range(1, levels):
                term = term + held[l] * perturbations[first + m, l].astype(F32)
            terms[m * rows : (m + 1) * rows, :] = term
        narrow = dot_split(terms[...], interp[...], ((1,), (1,)))
        narrow = sum_parts(narrow, lambda part: jnp.dot(share, part, preferred_element_type=F32))
        sent[pl.ds(pl.multiple_of(4 * first, 8), 4 * group), :] = scale * narrow

    if members <= GROUP:
        one_group(0)
    else:
        lax.fori_loop(0, members // GROUP, lambda g, c: (one_group(g * GROUP), c)[1], 0)


def member_kernel(received, member, rows_f, cols_f, gradient):
    coarse = rows_f.shape[0]
    main, following = [
        received[pl.ds(row, coarse, stride=4), :] + received[pl.ds(row + 2, coarse, stride=4), :] for row in range(2)
    ]
    at = iota(main.shape, 0)
    smooth = main + jnp.where(at == 0, 0.0, pltpu.roll(following, 1, 0))
    smooth = smooth + jnp.where(at == coarse - 1, following, 0.0)
    right_done = dot_precise(smooth, cols_f[...], ((1,), (1,)))
    gradient[0] = member[0] + dot_precise(rows_f[...], right_done, ((0,), (0,)))


def call(kernel, outs, scratch=(), results=(), staged=True):
    run = pl.pallas_call(
        kernel,
        out_shape=[
            jax.ShapeDtypeStruct(shape, dtype) if i in results else pltpu.VMEM(shape, dtype)
            for i, (shape, dtype) in enumerate(outs)
        ],
        scratch_shapes=[pltpu.VMEM(shape, dtype) for shape, dtype in scratch]
        + ([] if staged else [pltpu.SemaphoreType.DMA((7,))]),
        **({} if staged else {"in_specs": [pl.BlockSpec(memory_space=pltpu.HBM)] * 7}),
        cost_estimate=pl.CostEstimate(flops=100000, transcendentals=0, bytes_accessed=0),
        compiler_params=pltpu.CompilerParams(vmem_limit_bytes=VMEM_BYTES),
    )
    space = pltpu.VMEM if staged else pltpu.HBM
    return lambda *args: run(*[pltpu.with_memory_space_constraint(a, space) for a in args])


def on_device(
    member_control,
    static_control,
    perturbations,
    innovation,
    diffusivity,
    rows_factor,
    column_factor,
    ocean_mask,
    huber_blocks,
    fold_map,
):
    members, levels, rows, width = perturbations.shape
    wide, lev = lax.axis_size("wide"), lax.axis_size("lev")
    coarse_rows, coarse = rows_factor.shape[0], column_factor.shape[0]
    assert lev == 2 and members == wide and coarse_rows == wide and rows == 8 and levels >= STEPS
    ring_up = [(i, (i + 1) % wide) for i in range(wide)]
    ring_down = [(j, i) for i, j in ring_up]
    partner = [(0, 1), (1, 0)]
    cell = (levels, rows, width)

    swap, windows, value, kappa, member, rows_f, cols_f, blocks, fold = call(
        start_kernel,
        [
            (((2 * STEPS - 1) * rows, width), F32),
            ((2 * coarse_rows, coarse), F32),
            (cell, F32),
            (cell, F32),
            (member_control.shape, F32),
            (rows_factor.shape, F32),
            (column_factor.shape, F32),
            ((levels, coarse), jnp.int32),
            ((1, width), jnp.int32),
        ],
        staged=False,
    )(
        static_control,
        diffusivity,
        member_control,
        rows_factor,
        column_factor,
        huber_blocks.reshape(levels, coarse),
        fold_map.reshape(1, width),
    )
    swap = lax.ppermute(swap, "lev", partner)
    windows = lax.all_to_all(windows.reshape(wide, 2, coarse), "wide", 0, 0, tiled=True)
    windows = windows.reshape(2 * members, coarse)
    count = padded_rows(levels, True)
    up, down, interp, huber = call(
        pack_static_kernel,
        [((count, width), F32), ((count, width), F32), ((coarse, width), BF16), ((levels, width), F32)],
    )(value, kappa, swap, blocks)
    low = lax.ppermute(up, "wide", ring_up)
    high = lax.ppermute(down, "wide", ring_down)
    entries = levels + STEPS
    diffused, kappa_ext = call(
        static_kernel,
        [(cell, F32), ((entries - 1, 2 * rows, width), F32)],
        [((entries, 2 * rows, width), F32), (cell, F32), ((8, width), F32)],
    )(value, kappa, swap, low, high, fold)
    increment, weighted, scaled, swap = call(
        ensemble_kernel,
        [(cell, F32), (cell, F32), (cell, F32), ((STEPS * rows, width), F32)],
        [((2 * members, width), F32)],
    )(windows, interp, perturbations, diffused, innovation, kappa, ocean_mask, huber)
    swap = lax.ppermute(swap, "lev", partner)
    (sent,) = call(
        terms_kernel, [((4 * members, coarse), F32)], [((min(GROUP, members) * rows, width), F32)]
    )(perturbations, weighted, interp)
    received = lax.all_to_all(sent.reshape(2 * members, 2, coarse), ("wide", "lev"), 0, 0, tiled=True)
    received = received.reshape(4 * members, coarse)
    count = padded_rows(levels, False)
    up, down = call(pack_weighted_kernel, [((count, width), F32), ((count, width), F32)])(scaled, swap)
    low = lax.ppermute(up, "wide", ring_up)
    high = lax.ppermute(down, "wide", ring_down)
    (static_gradient,) = call(
        weighted_kernel,
        [(cell, F32)],
        [((entries, 2 * rows, width), F32), ((8, LANES), F32), (cell, F32), ((8, width), F32)],
        results=(0,),
    )(value, weighted, kappa, kappa_ext, scaled, swap, low, high, fold)
    (member_gradient,) = call(member_kernel, [(member_control.shape, F32)], results=(0,))(
        received, member, rows_f, cols_f
    )
    return (increment, member_gradient, static_gradient)


def solution(mesh):
    return jax.shard_map(
        on_device,
        mesh=mesh,
        in_specs=(
            P("wide", None, None),
            P("lev", "wide", None),
            P(None, "lev", "wide", None),
            P("lev", "wide", None),
            P("lev", "wide", None),
            P(),
            P(),
            P("wide", None),
            P("lev", "wide", None),
            P(),
        ),
        out_specs=(P("lev", "wide", None), P("wide", None, None), P("lev", "wide", None)),
        check_vma=False,
    )
```

```python
import inspect

import jax
import jax.numpy as jnp
from jax import lax
from jax.experimental import pallas as pl
from jax.experimental.pallas import tpu as pltpu
from jax.sharding import PartitionSpec as P


STEPS = 3
HUBER_EDGE = 1.0
VERTICAL_WEIGHT = 0.5
LANES = 128
GROUP = 16
VMEM_BYTES = 32 * 2**20
F32 = jnp.float32
BF16 = jnp.bfloat16


def dot(left, right, dims=((1,), (0,))):
    return lax.dot_general(left, right, (dims, ((), ())), preferred_element_type=F32)


def parts_of(array):
    high = array.astype(BF16)
    return high, (array - high.astype(F32)).astype(BF16)


def dot_precise(left, right, dims=((1,), (0,))):
    (left_high, left_low), (right_high, right_low) = parts_of(left), parts_of(right)
    return (dot(left_high, right_low, dims) + dot(left_low, right_high, dims)) + dot(left_high, right_high, dims)


def sum_parts(array, product):
    high, low = parts_of(array)
    return product(low) + product(high)


def dot_split(left, right, dims=((1,), (0,))):
    return sum_parts(left, lambda part: dot(part, right, dims))


def iota(shape, dim):
    return lax.broadcasted_iota(jnp.int32, shape, dim)


def level_at(entry, levels, lev):
    return jnp.where(lev == 0, entry, levels - 1 - entry)


def row_plan(levels, with_kappa):
    plan = [(False, d, e) for d in range(1, STEPS + 1) for e in range(levels + STEPS - d)]
    if with_kappa:
        plan += [(True, d, e) for d in range(1, STEPS) for e in range(levels + STEPS - 1 - d)]
    return plan


def padded_rows(levels, with_kappa):
    return -(-len(row_plan(levels, with_kappa)) // 8) * 8


def copies_of(sources, targets, done):
    return [pltpu.make_async_copy(s, t, done.at[i]) for i, (s, t) in enumerate(zip(sources, targets))]


def start_kernel(
    value_h, kappa_h, member_h, rows_h, cols_h, blocks_h, fold_h, swap, windows_h, value, kappa, member, rows_f, cols_f, blocks, fold, windows, done
):
    levels, rows, _ = value.shape
    coarse = rows_f.shape[0]
    lev = lax.axis_index("lev")
    sources = (member_h, cols_h, rows_h, kappa_h, value_h, blocks_h, fold_h)
    copies = copies_of(sources, (member, cols_f, rows_f, kappa, value, blocks, fold), done)
    for copy in copies:
        copy.start()
    for copy in copies[:3]:
        copy.wait()
    smoothed = dot_precise(rows_f[...], dot_precise(member[0], cols_f[...]))
    windows[pl.ds(0, coarse, stride=2), :] = smoothed
    ring = pltpu.roll(smoothed, coarse - 1, 0)
    windows[pl.ds(1, coarse, stride=2), :] = jnp.where(iota(smoothed.shape, 0) == coarse - 1, smoothed, ring)
    leave = pltpu.make_async_copy(windows, windows_h, done.at[len(copies)])
    leave.start()
    for copy in copies[3:]:
        copy.wait()
    for j in range(STEPS):
        at = level_at(levels - 1 - j, levels, lev)
        k = kappa[at]
        swap[j * rows : (j + 1) * rows, :] = jnp.sqrt(k) * value[at]
        if j < STEPS - 1:
            swap[(STEPS + j) * rows : (STEPS + j + 1) * rows, :] = k
    leave.wait()


def on_even():
    return lax.rem(lax.axis_index("wide"), 2) == 0


def pack_rows(plan, row_of, near, far, rows):
    def fill(upper, lower):
        for j, (is_kappa, d, e) in enumerate(plan):
            upper[j : j + 1, :] = row_of(is_kappa, e, rows - d)
            lower[j : j + 1, :] = row_of(is_kappa, e, d - 1)

    for out in (near, far):
        for j in range(len(plan), out.shape[0]):
            out[j : j + 1, :] = jnp.zeros((1, out.shape[1]), F32)
    even = on_even()
    pl.when(even)(lambda: fill(near, far))
    pl.when(jnp.logical_not(even))(lambda: fill(far, near))


def pack_static_kernel(value, kappa, swap, blocks, near, far, interp, huber):
    levels, rows, width = value.shape
    lev = lax.axis_index("lev")

    def row_of(is_kappa, e, r):
        if e >= levels:
            start = (e - levels + (STEPS if is_kappa else 0)) * rows
            return swap[start + r : start + r + 1, :]
        at = level_at(e, levels, lev)
        k = kappa[at, r : r + 1, :]
        return k if is_kappa else jnp.sqrt(k) * value[at, r : r + 1, :]

    pack_rows(row_plan(levels, True), row_of, near, far, rows)
    coarse = interp.shape[0]
    refine = width // coarse
    shape = (coarse, width)
    column = iota(shape, 1)
    at = iota(shape, 0)
    cell = column // refine
    fraction = (column % refine).astype(F32) * (1.0 / refine)
    following = jnp.where(cell == coarse - 1, 0, cell + 1)
    below = cell == at
    interp[...] = (
        jnp.where(below, 1.0 - fraction, 0.0) + jnp.where(following == at, fraction, 0.0)
    ).astype(BF16)
    spread = jnp.where(below, 1.0, 0.0).astype(BF16)
    huber[...] = jnp.dot(blocks[...].astype(F32).astype(BF16), spread, preferred_element_type=F32)


def pack_weighted_kernel(scaled, swap, near, far):
    levels, rows, _ = scaled.shape

    def row_of(is_kappa, e, r):
        if e >= levels:
            start = (e - levels) * rows
            return swap[start + r : start + r + 1, :]
        return scaled[e, r : r + 1, :]

    pack_rows(row_plan(levels, False), row_of, near, far, rows)


def unpack_rows(plan, state, kappa_ext, near, far, rows):
    def fill(low, high):
        is_first = lax.axis_index("wide") == 0
        for j, (is_kappa, d, e) in enumerate(plan):
            target = kappa_ext if is_kappa else state
            target[e, 2 * rows - d : 2 * rows - d + 1, :] = jnp.where(is_first, 0.0, low[j : j + 1, :])
            target[e, rows + d - 1 : rows + d, :] = high[j : j + 1, :]

    even = on_even()
    pl.when(even)(lambda: fill(far, near))
    pl.when(jnp.logical_not(even))(lambda: fill(near, far))


def diffuse_steps(state, kappa_ext, total, fold, edge, levels, rows, width, finish):
    is_last = lax.axis_index("wide") == lax.axis_size("wide") - 1
    tiles = width // LANES
    for step in range(STEPS):
        updated = levels + STEPS - 1 - step

        @pl.when(is_last)
        def _():
            for e in range(updated):
                edge[e : e + 1, :] = state[e, rows - 1 : rows, :]
            for t in range(tiles):
                index = jnp.broadcast_to(fold[:, t * LANES : (t + 1) * LANES], (8, LANES))
                lane = lax.rem(index, LANES)
                source = lax.div(index, LANES)
                found = jnp.zeros((8, LANES), F32)
                for q in range(tiles):
                    part = jnp.take_along_axis(
                        edge[:, q * LANES : (q + 1) * LANES], lane, axis=1, mode="promise_in_bounds"
                    )
                    found = jnp.where(source == q, part, found)
                for e in range(updated):
                    state[e, rows : rows + 1, t * LANES : (t + 1) * LANES] = found[e : e + 1, :]

        below = None
        for e in range(updated):
            whole = state[e]
            with_halo = step < STEPS - 1 and e < updated - 1
            kept = 2 * rows if with_halo else rows
            here = whole[:kept]
            above = state[e + 1, :kept, :]
            vertical = above if below is None else above + below[:kept]
            across = (
                pltpu.roll(whole, 2 * rows - 1, 0)[:kept]
                + pltpu.roll(whole, 1, 0)[:kept]
                + pltpu.roll(here, width - 1, 1)
                + pltpu.roll(here, 1, 1)
            )
            change = across + VERTICAL_WEIGHT * vertical - (4.0 + 2.0 * VERTICAL_WEIGHT) * here
            below = whole
            if step < STEPS - 1:
                state[e, :kept, :] = here + kappa_ext[e, :kept, :] * change
            if e < levels:
                if step == 0:
                    total[e] = change[:rows]
                elif step < STEPS - 1:
                    total[e] = total[e] + change[:rows]
                else:
                    finish(e, total[e] + change[:rows])


def static_kernel(value, kappa, swap, near, far, fold, diffused, kappa_ext, state, total, edge):
    levels, rows, width = value.shape
    lev = lax.axis_index("lev")
    zero = jnp.zeros((rows, width), F32)
    edge[...] = jnp.zeros(edge.shape, F32)
    for e in range(levels + STEPS):
        state[e, rows:, :] = zero
        if e < levels + STEPS - 1:
            kappa_ext[e, rows:, :] = zero
        if e < levels:
            at = level_at(e, levels, lev)
            k = kappa[at]
            kappa_ext[e, :rows, :] = k
            state[e, :rows, :] = jnp.sqrt(k) * value[at]
        else:
            start = (e - levels) * rows
            state[e, :rows, :] = swap[start : start + rows, :]
            if e < levels + STEPS - 1:
                start += STEPS * rows
                kappa_ext[e, :rows, :] = swap[start : start + rows, :]
    unpack_rows(row_plan(levels, True), state, kappa_ext, near, far, rows)

    def finish(e, change):
        at = level_at(e, levels, lev)
        diffused[at] = value[at] + jnp.sqrt(kappa[at]) * change

    diffuse_steps(state, kappa_ext, total, fold, edge, levels, rows, width, finish)


def weighted_kernel(
    value, weighted, kappa, kappa_ext, scaled, swap, near, far, fold, gradient_h, gradient, state, ring, total, edge, done
):
    levels, rows, width = value.shape
    lev = lax.axis_index("lev")
    zero = jnp.zeros((rows, width), F32)
    edge[...] = jnp.zeros(edge.shape, F32)
    for e in range(levels + STEPS):
        state[e, rows:, :] = zero
        if e < levels:
            state[e, :rows, :] = scaled[e]
        else:
            start = (e - levels) * rows
            state[e, :rows, :] = swap[start : start + rows, :]
    unpack_rows(row_plan(levels, False), state, ring, near, far, rows)

    def finish(e, change):
        at = level_at(e, levels, lev)
        gradient[e] = value[at] + (weighted[at] + jnp.sqrt(kappa[at]) * change)
        copy = pltpu.make_async_copy(gradient.at[e], gradient_h.at[at], done.at[e])
        copy.start()
        leaving.append(copy)

    leaving = []
    diffuse_steps(state, kappa_ext, total, fold, edge, levels, rows, width, finish)
    for copy in leaving:
        copy.wait()


def ensemble_kernel(
    windows, interp, perturbations, diffused, innovation, kappa, mask, huber, increment, weighted, scaled, swap, sent_h, sent, coarse, terms, done
):
    members, levels, rows, width = perturbations.shape
    lev = lax.axis_index("lev")
    coarse[...] = dot_split(windows[...], interp[...])
    fraction = iota((rows, width), 0).astype(F32) * (1.0 / rows)

    def add_group(first, sums):
        sums = list(sums)
        for m in range(min(GROUP, members)):
            at = first + m
            fine = (1.0 - fraction) * coarse[pl.ds(2 * at, 1), :] + fraction * coarse[pl.ds(2 * at + 1, 1), :]
            for l in range(levels):
                sums[l] = sums[l] + fine * perturbations[at, l].astype(F32)
        return tuple(sums)

    sums = tuple(jnp.zeros((rows, width), F32) for _ in range(levels))
    if members <= GROUP:
        sums = add_group(0, sums)
    else:
        sums = lax.fori_loop(0, members // GROUP, lambda g, s: add_group(g * GROUP, s), sums)
    ocean = mask[...].astype(F32)
    scale = (members - 1) ** (-0.5)
    for l in range(levels):
        grown = ocean * (scale * sums[l] + diffused[l])
        increment[l] = grown
        misfit = grown - innovation[l]
        weight = jnp.where(
            huber[l : l + 1, :] > 0.5, HUBER_EDGE / jnp.maximum(jnp.abs(misfit), HUBER_EDGE), 1.0
        )
        weighted[l] = ocean * weight * misfit
    member_terms(perturbations, weighted, interp, sent, terms)
    leave = pltpu.make_async_copy(sent, sent_h, done.at[0])
    leave.start()
    for l in range(levels):
        rooted = jnp.sqrt(kappa[l]) * weighted[l]
        entry = level_at(l, levels, lev)
        scaled[entry] = rooted

        @pl.when(entry > 0)
        def _():
            swap[pl.ds(pl.multiple_of((levels - 1 - entry) * rows, 8), rows), :] = rooted

    leave.wait()


def member_terms(perturbations, weighted, interp, sent, terms):
    members, levels, rows, _ = perturbations.shape
    group = min(GROUP, members)
    scale = (members - 1) ** (-0.5)
    shape = (4 * group, group * rows)
    pair = iota(shape, 0)
    column = iota(shape, 1)
    fraction = (column % rows).astype(F32) * (1.0 / rows)
    share = jnp.where(pair % 2 == 0, 1.0 - fraction, fraction)
    share = jnp.where(column // rows == pair // 4, share, 0.0).astype(BF16)
    held = [weighted[l] for l in range(levels)]

    def one_group(first):
        for m in range(group):
            term = held[0] * perturbations[first + m, 0].astype(F32)
            for l in range(1, levels):
                term = term + held[l] * perturbations[first + m, l].astype(F32)
            terms[m * rows : (m + 1) * rows, :] = term
        narrow = dot_split(terms[...], interp[...], ((1,), (1,)))
        narrow = sum_parts(narrow, lambda part: dot(share, part))
        sent[pl.ds(pl.multiple_of(4 * first, 8), 4 * group), :] = scale * narrow

    if members <= GROUP:
        one_group(0)
    else:
        lax.fori_loop(0, members // GROUP, lambda g, c: (one_group(g * GROUP), c)[1], 0)


def member_kernel(received, member, rows_f, cols_f, gradient):
    coarse = rows_f.shape[0]
    main, following = [
        received[pl.ds(row, coarse, stride=4), :] + received[pl.ds(row + 2, coarse, stride=4), :] for row in range(2)
    ]
    at = iota(main.shape, 0)
    smooth = main + jnp.where(at == 0, 0.0, pltpu.roll(following, 1, 0))
    smooth = smooth + jnp.where(at == coarse - 1, following, 0.0)
    right_done = dot_precise(smooth, cols_f[...], ((1,), (1,)))
    gradient[0] = member[0] + dot_precise(rows_f[...], right_done, ((0,), (0,)))


def call(kernel, outs, scratch=(), results=()):
    names = [n for n in inspect.signature(kernel).parameters]
    count = len(names) - len(outs) - len(scratch)
    in_hbm = [n.endswith("_h") for n in names]

    def out_type(i, shape, dtype):
        if i in results:
            return jax.ShapeDtypeStruct(shape, dtype)
        return (pltpu.HBM if in_hbm[count + i] else pltpu.VMEM)(shape, dtype)

    def spec(hbm):
        return pl.BlockSpec(memory_space=pltpu.HBM if hbm else pltpu.VMEM)

    run = pl.pallas_call(
        kernel,
        in_specs=[spec(in_hbm[i]) for i in range(count)],
        out_specs=[spec(in_hbm[count + i]) for i in range(len(outs))],
        out_shape=[out_type(i, shape, dtype) for i, (shape, dtype) in enumerate(outs)],
        scratch_shapes=[
            pltpu.SemaphoreType.DMA(shape) if dtype is None else pltpu.VMEM(shape, dtype) for shape, dtype in scratch
        ],
        cost_estimate=pl.CostEstimate(flops=100000, transcendentals=0, bytes_accessed=0),
        compiler_params=pltpu.CompilerParams(vmem_limit_bytes=VMEM_BYTES),
    )

    def place(args):
        return [pltpu.with_memory_space_constraint(a, pltpu.HBM if in_hbm[i] else pltpu.VMEM) for i, a in enumerate(args)]

    return lambda *args: run(*place(args))


def on_device(
    member_control,
    static_control,
    perturbations,
    innovation,
    diffusivity,
    rows_factor,
    column_factor,
    ocean_mask,
    huber_blocks,
    fold_map,
):
    members, levels, rows, width = perturbations.shape
    wide, lev = lax.axis_size("wide"), lax.axis_size("lev")
    coarse_rows, coarse = rows_factor.shape[0], column_factor.shape[0]
    assert lev == 2 and members == wide and coarse_rows == wide and rows == 8 and levels >= STEPS
    assert wide % 2 == 0
    pairs = [(i, i ^ 1) for i in range(wide)]
    between = [(0, 0), (wide - 1, wide - 1)]
    for i in range(1, wide - 1, 2):
        between += [(i, i + 1), (i + 1, i)]
    partner = [(0, 1), (1, 0)]
    cell = (levels, rows, width)

    swap, windows, value, kappa, member, rows_f, cols_f, blocks, fold = call(
        start_kernel,
        [
            (((2 * STEPS - 1) * rows, width), F32),
            ((2 * coarse_rows, coarse), F32),
            (cell, F32),
            (cell, F32),
            (member_control.shape, F32),
            (rows_factor.shape, F32),
            (column_factor.shape, F32),
            ((levels, coarse), jnp.int32),
            ((1, width), jnp.int32),
        ],
        [((2 * coarse_rows, coarse), F32), ((8,), None)],
    )(
        static_control,
        diffusivity,
        member_control,
        rows_factor,
        column_factor,
        huber_blocks.reshape(levels, coarse),
        fold_map.reshape(1, width),
    )
    swap = lax.ppermute(swap, "lev", partner)
    windows = lax.all_to_all(windows.reshape(wide, 2, coarse), "wide", 0, 0, tiled=True)
    windows = windows.reshape(2 * members, coarse)
    count = padded_rows(levels, True)
    near, far, interp, huber = call(
        pack_static_kernel,
        [((count, width), F32), ((count, width), F32), ((coarse, width), BF16), ((levels, width), F32)],
    )(value, kappa, swap, blocks)
    far = lax.ppermute(far, "wide", between)
    near = lax.ppermute(near, "wide", pairs)
    entries = levels + STEPS
    diffused, kappa_ext = call(
        static_kernel,
        [(cell, F32), ((entries - 1, 2 * rows, width), F32)],
        [((entries, 2 * rows, width), F32), (cell, F32), ((8, width), F32)],
    )(value, kappa, swap, near, far, fold)
    increment, weighted, scaled, swap, sent = call(
        ensemble_kernel,
        [(cell, F32), (cell, F32), (cell, F32), ((STEPS * rows, width), F32), ((4 * members, coarse), F32)],
        [
            ((4 * members, coarse), F32),
            ((2 * members, width), F32),
            ((min(GROUP, members) * rows, width), F32),
            ((1,), None),
        ],
    )(windows, interp, perturbations, diffused, innovation, kappa, ocean_mask, huber)
    swap = lax.ppermute(swap, "lev", partner)
    received = lax.all_to_all(sent.reshape(2 * members, 2, coarse), ("wide", "lev"), 0, 0, tiled=True)
    received = received.reshape(4 * members, coarse)
    count = padded_rows(levels, False)
    near, far = call(pack_weighted_kernel, [((count, width), F32), ((count, width), F32)])(scaled, swap)
    far = lax.ppermute(far, "wide", between)
    near = lax.ppermute(near, "wide", pairs)
    (static_gradient,) = call(
        weighted_kernel,
        [(cell, F32)],
        [
            (cell, F32),
            ((entries, 2 * rows, width), F32),
            ((8, LANES), F32),
            (cell, F32),
            ((8, width), F32),
            ((levels,), None),
        ],
    )(value, weighted, kappa, kappa_ext, scaled, swap, near, far, fold)
    (member_gradient,) = call(member_kernel, [(member_control.shape, F32)], results=(0,))(
        received, member, rows_f, cols_f
    )
    return (increment, member_gradient, static_gradient)


def solution(mesh):
    return jax.shard_map(
        on_device,
        mesh=mesh,
        in_specs=(
            P("wide", None, None),
            P("lev", "wide", None),
            P(None, "lev", "wide", None),
            P("lev", "wide", None),
            P("lev", "wide", None),
            P(),
            P(),
            P("wide", None),
            P("lev", "wide", None),
            P(),
        ),
        out_specs=(P("lev", "wide", None), P("wide", None, None), P("lev", "wide", None)),
        check_vma=False,
    )
```

```python
import inspect

import jax
import jax.numpy as jnp
from jax import lax
from jax.experimental import pallas as pl
from jax.experimental.pallas import tpu as pltpu
from jax.sharding import PartitionSpec as P


STEPS = 3
HUBER_EDGE = 1.0
VERTICAL_WEIGHT = 0.5
LANES = 128
GROUP = 16
VMEM_BYTES = 32 * 2**20
F32 = jnp.float32
BF16 = jnp.bfloat16


def dot(left, right, dims=((1,), (0,))):
    return lax.dot_general(left, right, (dims, ((), ())), preferred_element_type=F32)


def parts_of(array):
    high = array.astype(BF16)
    return high, (array - high.astype(F32)).astype(BF16)


def dot_precise(left, right, dims=((1,), (0,))):
    (left_high, left_low), (right_high, right_low) = parts_of(left), parts_of(right)
    return (dot(left_high, right_low, dims) + dot(left_low, right_high, dims)) + dot(left_high, right_high, dims)


def sum_parts(array, product):
    high, low = parts_of(array)
    return product(low) + product(high)


def dot_split(left, right, dims=((1,), (0,))):
    return sum_parts(left, lambda part: dot(part, right, dims))


def iota(shape, dim):
    return lax.broadcasted_iota(jnp.int32, shape, dim)


def level_at(entry, levels, lev):
    return jnp.where(lev == 0, entry, levels - 1 - entry)


def row_plan(levels, with_kappa):
    plan = [(False, d, e) for d in range(1, STEPS + 1) for e in range(levels + STEPS - d)]
    if with_kappa:
        plan += [(True, d, e) for d in range(1, STEPS) for e in range(levels + STEPS - 1 - d)]
    return plan


def padded_rows(levels, with_kappa):
    return -(-len(row_plan(levels, with_kappa)) // 8) * 8


def copies_of(sources, targets, done):
    return [pltpu.make_async_copy(s, t, done.at[i]) for i, (s, t) in enumerate(zip(sources, targets))]


def start_kernel(
    value_h, kappa_h, member_h, rows_h, cols_h, blocks_h, fold_h, swap, windows_h, value, kappa, member, rows_f, cols_f, blocks, fold, windows, done
):
    levels, rows, _ = value.shape
    coarse = rows_f.shape[0]
    lev = lax.axis_index("lev")
    sources = (member_h, cols_h, rows_h, kappa_h, value_h, blocks_h, fold_h)
    copies = copies_of(sources, (member, cols_f, rows_f, kappa, value, blocks, fold), done)
    for copy in copies:
        copy.start()
    for copy in copies[:3]:
        copy.wait()
    smoothed = dot_precise(rows_f[...], dot_precise(member[0], cols_f[...]))
    following = jnp.where(iota(smoothed.shape, 0) == coarse - 1, smoothed, pltpu.roll(smoothed, coarse - 1, 0))
    mine = jnp.where(lev == 0, smoothed, following)
    for target in range(2):
        windows[target * coarse : (target + 1) * coarse, :] = mine
    leave = pltpu.make_async_copy(windows, windows_h, done.at[len(copies)])
    leave.start()
    for copy in copies[3:]:
        copy.wait()
    for j in range(STEPS):
        at = level_at(levels - 1 - j, levels, lev)
        k = kappa[at]
        swap[j * rows : (j + 1) * rows, :] = jnp.sqrt(k) * value[at]
        if j < STEPS - 1:
            swap[(STEPS + j) * rows : (STEPS + j + 1) * rows, :] = k
    leave.wait()


def on_even():
    return lax.rem(lax.axis_index("wide"), 2) == 0


def pack_rows(plan, row_of, near, far, rows):
    def fill(upper, lower):
        for j, (is_kappa, d, e) in enumerate(plan):
            upper[j : j + 1, :] = row_of(is_kappa, e, rows - d)
            lower[j : j + 1, :] = row_of(is_kappa, e, d - 1)

    for out in (near, far):
        for j in range(len(plan), out.shape[0]):
            out[j : j + 1, :] = jnp.zeros((1, out.shape[1]), F32)
    even = on_even()
    pl.when(even)(lambda: fill(near, far))
    pl.when(jnp.logical_not(even))(lambda: fill(far, near))


def pack_static_kernel(value, kappa, swap, near, far):
    levels, rows, _ = value.shape
    lev = lax.axis_index("lev")

    def row_of(is_kappa, e, r):
        if e >= levels:
            start = (e - levels + (STEPS if is_kappa else 0)) * rows
            return swap[start + r : start + r + 1, :]
        at = level_at(e, levels, lev)
        k = kappa[at, r : r + 1, :]
        return k if is_kappa else jnp.sqrt(k) * value[at, r : r + 1, :]

    pack_rows(row_plan(levels, True), row_of, near, far, rows)


def prepare_kernel(blocks, perturbations_h, innovation_h, mask_h, interp, huber, perturbations, innovation, mask, done):
    copies = copies_of((perturbations_h, innovation_h, mask_h), (perturbations, innovation, mask), done)
    for copy in copies:
        copy.start()
    width = interp.shape[1]
    coarse = interp.shape[0]
    refine = width // coarse
    shape = (coarse, width)
    column = iota(shape, 1)
    at = iota(shape, 0)
    cell = column // refine
    fraction = (column % refine).astype(F32) * (1.0 / refine)
    following = jnp.where(cell == coarse - 1, 0, cell + 1)
    below = cell == at
    interp[...] = (
        jnp.where(below, 1.0 - fraction, 0.0) + jnp.where(following == at, fraction, 0.0)
    ).astype(BF16)
    spread = jnp.where(below, 1.0, 0.0).astype(BF16)
    huber[...] = jnp.dot(blocks[...].astype(F32).astype(BF16), spread, preferred_element_type=F32)
    for copy in copies:
        copy.wait()


def pack_weighted_kernel(scaled, swap, near, far):
    levels, rows, _ = scaled.shape

    def row_of(is_kappa, e, r):
        if e >= levels:
            start = (e - levels) * rows
            return swap[start + r : start + r + 1, :]
        return scaled[e, r : r + 1, :]

    pack_rows(row_plan(levels, False), row_of, near, far, rows)


def unpack_rows(plan, state, kappa_ext, near, far, rows):
    def fill(low, high):
        is_first = lax.axis_index("wide") == 0
        for j, (is_kappa, d, e) in enumerate(plan):
            target = kappa_ext if is_kappa else state
            target[e, 2 * rows - d : 2 * rows - d + 1, :] = jnp.where(is_first, 0.0, low[j : j + 1, :])
            target[e, rows + d - 1 : rows + d, :] = high[j : j + 1, :]

    even = on_even()
    pl.when(even)(lambda: fill(far, near))
    pl.when(jnp.logical_not(even))(lambda: fill(near, far))


def diffuse_steps(state, kappa_ext, total, fold, edge, levels, rows, width, finish):
    is_last = lax.axis_index("wide") == lax.axis_size("wide") - 1
    tiles = width // LANES
    for step in range(STEPS):
        updated = levels + STEPS - 1 - step

        @pl.when(is_last)
        def _():
            for e in range(updated):
                edge[e : e + 1, :] = state[e, rows - 1 : rows, :]
            for t in range(tiles):
                index = jnp.broadcast_to(fold[:, t * LANES : (t + 1) * LANES], (8, LANES))
                lane = lax.rem(index, LANES)
                source = lax.div(index, LANES)
                found = jnp.zeros((8, LANES), F32)
                for q in range(tiles):
                    part = jnp.take_along_axis(
                        edge[:, q * LANES : (q + 1) * LANES], lane, axis=1, mode="promise_in_bounds"
                    )
                    found = jnp.where(source == q, part, found)
                for e in range(updated):
                    state[e, rows : rows + 1, t * LANES : (t + 1) * LANES] = found[e : e + 1, :]

        below = None
        for e in range(updated):
            whole = state[e]
            with_halo = step < STEPS - 1 and e < updated - 1
            kept = 2 * rows if with_halo else rows
            here = whole[:kept]
            above = state[e + 1, :kept, :]
            vertical = above if below is None else above + below[:kept]
            across = (
                pltpu.roll(whole, 2 * rows - 1, 0)[:kept]
                + pltpu.roll(whole, 1, 0)[:kept]
                + pltpu.roll(here, width - 1, 1)
                + pltpu.roll(here, 1, 1)
            )
            change = across + VERTICAL_WEIGHT * vertical - (4.0 + 2.0 * VERTICAL_WEIGHT) * here
            below = whole
            if step < STEPS - 1:
                state[e, :kept, :] = here + kappa_ext[e, :kept, :] * change
            if e < levels:
                if step == 0:
                    total[e] = change[:rows]
                elif step < STEPS - 1:
                    total[e] = total[e] + change[:rows]
                else:
                    finish(e, total[e] + change[:rows])


def static_kernel(value, kappa, swap, near, far, fold, diffused, kappa_ext, state, total, edge):
    levels, rows, width = value.shape
    lev = lax.axis_index("lev")
    zero = jnp.zeros((rows, width), F32)
    edge[...] = jnp.zeros(edge.shape, F32)
    for e in range(levels + STEPS):
        state[e, rows:, :] = zero
        if e < levels + STEPS - 1:
            kappa_ext[e, rows:, :] = zero
        if e < levels:
            at = level_at(e, levels, lev)
            k = kappa[at]
            kappa_ext[e, :rows, :] = k
            state[e, :rows, :] = jnp.sqrt(k) * value[at]
        else:
            start = (e - levels) * rows
            state[e, :rows, :] = swap[start : start + rows, :]
            if e < levels + STEPS - 1:
                start += STEPS * rows
                kappa_ext[e, :rows, :] = swap[start : start + rows, :]
    unpack_rows(row_plan(levels, True), state, kappa_ext, near, far, rows)

    def finish(e, change):
        at = level_at(e, levels, lev)
        diffused[at] = value[at] + jnp.sqrt(kappa[at]) * change

    diffuse_steps(state, kappa_ext, total, fold, edge, levels, rows, width, finish)


def weighted_kernel(
    value, weighted, kappa, kappa_ext, scaled, swap, near, far, fold, gradient_h, gradient, state, ring, total, edge, done
):
    levels, rows, width = value.shape
    lev = lax.axis_index("lev")
    zero = jnp.zeros((rows, width), F32)
    edge[...] = jnp.zeros(edge.shape, F32)
    for e in range(levels + STEPS):
        state[e, rows:, :] = zero
        if e < levels:
            state[e, :rows, :] = scaled[e]
        else:
            start = (e - levels) * rows
            state[e, :rows, :] = swap[start : start + rows, :]
    unpack_rows(row_plan(levels, False), state, ring, near, far, rows)

    def finish(e, change):
        at = level_at(e, levels, lev)
        gradient[e] = value[at] + (weighted[at] + jnp.sqrt(kappa[at]) * change)
        copy = pltpu.make_async_copy(gradient.at[e], gradient_h.at[at], done.at[e])
        copy.start()
        leaving.append(copy)

    leaving = []
    diffuse_steps(state, kappa_ext, total, fold, edge, levels, rows, width, finish)
    for copy in leaving:
        copy.wait()


def ensemble_kernel(
    windows, interp, perturbations, diffused, innovation, kappa, mask, huber, increment, weighted, scaled, swap, sent_h, sent, coarse, terms, done
):
    members, levels, rows, width = perturbations.shape
    lev = lax.axis_index("lev")
    coarse[...] = dot_split(windows[...], interp[...])
    fraction = iota((rows, width), 0).astype(F32) * (1.0 / rows)

    def add_group(first, sums):
        sums = list(sums)
        for m in range(min(GROUP, members)):
            at = first + m
            fine = (1.0 - fraction) * coarse[pl.ds(at, 1), :] + fraction * coarse[pl.ds(members + at, 1), :]
            for l in range(levels):
                sums[l] = sums[l] + fine * perturbations[at, l].astype(F32)
        return tuple(sums)

    sums = tuple(jnp.zeros((rows, width), F32) for _ in range(levels))
    if members <= GROUP:
        sums = add_group(0, sums)
    else:
        sums = lax.fori_loop(0, members // GROUP, lambda g, s: add_group(g * GROUP, s), sums)
    ocean = mask[...].astype(F32)
    scale = (members - 1) ** (-0.5)
    for l in range(levels):
        grown = ocean * (scale * sums[l] + diffused[l])
        increment[l] = grown
        misfit = grown - innovation[l]
        weight = jnp.where(
            huber[l : l + 1, :] > 0.5, HUBER_EDGE / jnp.maximum(jnp.abs(misfit), HUBER_EDGE), 1.0
        )
        weighted[l] = ocean * weight * misfit
    member_terms(perturbations, weighted, interp, sent, terms)
    leave = pltpu.make_async_copy(sent, sent_h, done.at[0])
    leave.start()
    for l in range(levels):
        rooted = jnp.sqrt(kappa[l]) * weighted[l]
        entry = level_at(l, levels, lev)
        scaled[entry] = rooted

        @pl.when(entry > 0)
        def _():
            swap[pl.ds(pl.multiple_of((levels - 1 - entry) * rows, 8), rows), :] = rooted

    leave.wait()


def member_terms(perturbations, weighted, interp, sent, terms):
    members, levels, rows, _ = perturbations.shape
    group = min(GROUP, members)
    scale = (members - 1) ** (-0.5)
    shape = (2 * group, group * rows)
    pair = iota(shape, 0)
    column = iota(shape, 1)
    fraction = (column % rows).astype(F32) * (1.0 / rows)
    share = jnp.where(pair % 2 == 0, 1.0 - fraction, fraction)
    share = jnp.where(column // rows == pair // 2, share, 0.0).astype(BF16)
    held = [weighted[l] for l in range(levels)]

    def one_group(first):
        for m in range(group):
            term = held[0] * perturbations[first + m, 0].astype(F32)
            for l in range(1, levels):
                term = term + held[l] * perturbations[first + m, l].astype(F32)
            terms[m * rows : (m + 1) * rows, :] = term
        narrow = dot_split(terms[...], interp[...], ((1,), (1,)))
        narrow = sum_parts(narrow, lambda part: dot(share, part))
        for target in range(2):
            start = pl.multiple_of(2 * (target * members + first), 8)
            sent[pl.ds(start, 2 * group), :] = scale * narrow

    if members <= GROUP:
        one_group(0)
    else:
        lax.fori_loop(0, members // GROUP, lambda g, c: (one_group(g * GROUP), c)[1], 0)


def member_kernel(received, member, rows_f, cols_f, gradient):
    coarse = rows_f.shape[0]
    main, following = [
        received[pl.ds(row, coarse, stride=2), :] + received[pl.ds(2 * coarse + row, coarse, stride=2), :] for row in range(2)
    ]
    at = iota(main.shape, 0)
    smooth = main + jnp.where(at == 0, 0.0, pltpu.roll(following, 1, 0))
    smooth = smooth + jnp.where(at == coarse - 1, following, 0.0)
    right_done = dot_precise(smooth, cols_f[...], ((1,), (1,)))
    gradient[0] = member[0] + dot_precise(rows_f[...], right_done, ((0,), (0,)))


def call(kernel, outs, scratch=(), results=()):
    names = [n for n in inspect.signature(kernel).parameters]
    count = len(names) - len(outs) - len(scratch)
    in_hbm = [n.endswith("_h") for n in names]

    def out_type(i, shape, dtype):
        if i in results:
            return jax.ShapeDtypeStruct(shape, dtype)
        return (pltpu.HBM if in_hbm[count + i] else pltpu.VMEM)(shape, dtype)

    def spec(hbm):
        return pl.BlockSpec(memory_space=pltpu.HBM if hbm else pltpu.VMEM)

    run = pl.pallas_call(
        kernel,
        in_specs=[spec(in_hbm[i]) for i in range(count)],
        out_specs=[spec(in_hbm[count + i]) for i in range(len(outs))],
        out_shape=[out_type(i, shape, dtype) for i, (shape, dtype) in enumerate(outs)],
        scratch_shapes=[
            pltpu.SemaphoreType.DMA(shape) if dtype is None else pltpu.VMEM(shape, dtype) for shape, dtype in scratch
        ],
        cost_estimate=pl.CostEstimate(flops=100000, transcendentals=0, bytes_accessed=0),
        compiler_params=pltpu.CompilerParams(vmem_limit_bytes=VMEM_BYTES),
    )

    def place(args):
        return [pltpu.with_memory_space_constraint(a, pltpu.HBM if in_hbm[i] else pltpu.VMEM) for i, a in enumerate(args)]

    return lambda *args: run(*place(args))


def on_device(
    member_control,
    static_control,
    perturbations,
    innovation,
    diffusivity,
    rows_factor,
    column_factor,
    ocean_mask,
    huber_blocks,
    fold_map,
):
    members, levels, rows, width = perturbations.shape
    wide, lev = lax.axis_size("wide"), lax.axis_size("lev")
    coarse_rows, coarse = rows_factor.shape[0], column_factor.shape[0]
    assert lev == 2 and members == wide and coarse_rows == wide and rows == 8 and levels >= STEPS
    assert wide % 2 == 0
    pairs = [(i, i ^ 1) for i in range(wide)]
    between = [(0, 0), (wide - 1, wide - 1)]
    for i in range(1, wide - 1, 2):
        between += [(i, i + 1), (i + 1, i)]
    partner = [(0, 1), (1, 0)]
    cell = (levels, rows, width)

    swap, windows, value, kappa, member, rows_f, cols_f, blocks, fold = call(
        start_kernel,
        [
            (((2 * STEPS - 1) * rows, width), F32),
            ((2 * coarse_rows, coarse), F32),
            (cell, F32),
            (cell, F32),
            (member_control.shape, F32),
            (rows_factor.shape, F32),
            (column_factor.shape, F32),
            ((levels, coarse), jnp.int32),
            ((1, width), jnp.int32),
        ],
        [((2 * coarse_rows, coarse), F32), ((8,), None)],
    )(
        static_control,
        diffusivity,
        member_control,
        rows_factor,
        column_factor,
        huber_blocks.reshape(levels, coarse),
        fold_map.reshape(1, width),
    )
    swap = lax.ppermute(swap, "lev", partner)
    windows = lax.all_to_all(windows.reshape(2 * wide, 1, coarse), ("lev", "wide"), 0, 0, tiled=True)
    windows = windows.reshape(2 * members, coarse)
    count = padded_rows(levels, True)
    near, far = call(pack_static_kernel, [((count, width), F32), ((count, width), F32)])(value, kappa, swap)
    far = lax.ppermute(far, "wide", between)
    near = lax.ppermute(near, "wide", pairs)
    interp, huber, perturbations, innovation, mask = call(
        prepare_kernel,
        [
            ((coarse, width), BF16),
            ((levels, width), F32),
            (perturbations.shape, BF16),
            (cell, F32),
            (ocean_mask.shape, jnp.int32),
        ],
        [((3,), None)],
    )(blocks, perturbations, innovation, ocean_mask)
    entries = levels + STEPS
    diffused, kappa_ext = call(
        static_kernel,
        [(cell, F32), ((entries - 1, 2 * rows, width), F32)],
        [((entries, 2 * rows, width), F32), (cell, F32), ((8, width), F32)],
    )(value, kappa, swap, near, far, fold)
    increment, weighted, scaled, swap, sent = call(
        ensemble_kernel,
        [(cell, F32), (cell, F32), (cell, F32), ((STEPS * rows, width), F32), ((4 * members, coarse), F32)],
        [
            ((4 * members, coarse), F32),
            ((2 * members, width), F32),
            ((min(GROUP, members) * rows, width), F32),
            ((1,), None),
        ],
    )(windows, interp, perturbations, diffused, innovation, kappa, mask, huber)
    swap = lax.ppermute(swap, "lev", partner)
    received = lax.all_to_all(sent.reshape(2 * members, 2, coarse), ("lev", "wide"), 0, 0, tiled=True)
    received = received.reshape(4 * members, coarse)
    count = padded_rows(levels, False)
    near, far = call(pack_weighted_kernel, [((count, width), F32), ((count, width), F32)])(scaled, swap)
    far = lax.ppermute(far, "wide", between)
    near = lax.ppermute(near, "wide", pairs)
    (static_gradient,) = call(
        weighted_kernel,
        [(cell, F32)],
        [
            (cell, F32),
            ((entries, 2 * rows, width), F32),
            ((8, LANES), F32),
            (cell, F32),
            ((8, width), F32),
            ((levels,), None),
        ],
    )(value, weighted, kappa, kappa_ext, scaled, swap, near, far, fold)
    (member_gradient,) = call(member_kernel, [(member_control.shape, F32)], results=(0,))(
        received, member, rows_f, cols_f
    )
    return (increment, member_gradient, static_gradient)


def solution(mesh):
    return jax.shard_map(
        on_device,
        mesh=mesh,
        in_specs=(
            P("wide", None, None),
            P("lev", "wide", None),
            P(None, "lev", "wide", None),
            P("lev", "wide", None),
            P("lev", "wide", None),
            P(),
            P(),
            P("wide", None),
            P("lev", "wide", None),
            P(),
        ),
        out_specs=(P("lev", "wide", None), P("wide", None, None), P("lev", "wide", None)),
        check_vma=False,
    )
```

```python
import inspect

import jax
import jax.numpy as jnp
from jax import lax
from jax.experimental import pallas as pl
from jax.experimental.pallas import tpu as pltpu
from jax.sharding import PartitionSpec as P


STEPS = 3
HUBER_EDGE = 1.0
VERTICAL_WEIGHT = 0.5
LANES = 128
GROUP = 16
VMEM_BYTES = 32 * 2**20
F32 = jnp.float32
BF16 = jnp.bfloat16


def dot(left, right, dims=((1,), (0,))):
    return lax.dot_general(left, right, (dims, ((), ())), preferred_element_type=F32)


def parts_of(array):
    high = array.astype(BF16)
    return high, (array - high.astype(F32)).astype(BF16)


def dot_precise(left, right, dims=((1,), (0,))):
    (left_high, left_low), (right_high, right_low) = parts_of(left), parts_of(right)
    return (dot(left_high, right_low, dims) + dot(left_low, right_high, dims)) + dot(left_high, right_high, dims)


def sum_parts(array, product):
    high, low = parts_of(array)
    return product(low) + product(high)


def dot_split(left, right, dims=((1,), (0,))):
    return sum_parts(left, lambda part: dot(part, right, dims))


def iota(shape, dim):
    return lax.broadcasted_iota(jnp.int32, shape, dim)


def level_at(entry, levels, lev):
    return jnp.where(lev == 0, entry, levels - 1 - entry)


def row_plan(levels, with_kappa):
    plan = [(False, d, e) for d in range(1, STEPS + 1) for e in range(levels + STEPS - d)]
    if with_kappa:
        plan += [(True, d, e) for d in range(1, STEPS) for e in range(levels + STEPS - 1 - d)]
    return plan


def padded_rows(levels, with_kappa):
    return -(-len(row_plan(levels, with_kappa)) // 8) * 8


def copies_of(sources, targets, done):
    return [pltpu.make_async_copy(s, t, done.at[i]) for i, (s, t) in enumerate(zip(sources, targets))]


def start_kernel(
    value_h, kappa_h, member_h, rows_h, cols_h, blocks_h, fold_h, swap, windows_h, value, kappa, member, rows_f, cols_f, blocks, fold, windows, done
):
    levels, rows, _ = value.shape
    coarse = rows_f.shape[0]
    lev = lax.axis_index("lev")
    sources = (member_h, cols_h, rows_h, kappa_h, value_h, blocks_h, fold_h)
    copies = copies_of(sources, (member, cols_f, rows_f, kappa, value, blocks, fold), done)
    for copy in copies:
        copy.start()
    for copy in copies[:3]:
        copy.wait()
    smoothed = dot_precise(rows_f[...], dot_precise(member[0], cols_f[...]))
    following = jnp.where(iota(smoothed.shape, 0) == coarse - 1, smoothed, pltpu.roll(smoothed, coarse - 1, 0))
    mine = jnp.where(lev == 0, smoothed, following)
    for target in range(2):
        windows[target * coarse : (target + 1) * coarse, :] = mine
    leave = pltpu.make_async_copy(windows, windows_h, done.at[len(copies)])
    leave.start()
    for copy in copies[3:]:
        copy.wait()
    for j in range(STEPS):
        at = level_at(levels - 1 - j, levels, lev)
        k = kappa[at]
        swap[j * rows : (j + 1) * rows, :] = jnp.sqrt(k) * value[at]
        if j < STEPS - 1:
            swap[(STEPS + j) * rows : (STEPS + j + 1) * rows, :] = k
    leave.wait()


def on_even():
    return lax.rem(lax.axis_index("wide"), 2) == 0


def pack_rows(plan, row_of, near, far, rows):
    def fill(upper, lower):
        for j, (is_kappa, d, e) in enumerate(plan):
            upper[j : j + 1, :] = row_of(is_kappa, e, rows - d)
            lower[j : j + 1, :] = row_of(is_kappa, e, d - 1)

    for out in (near, far):
        for j in range(len(plan), out.shape[0]):
            out[j : j + 1, :] = jnp.zeros((1, out.shape[1]), F32)
    even = on_even()
    pl.when(even)(lambda: fill(near, far))
    pl.when(jnp.logical_not(even))(lambda: fill(far, near))


def pack_static_kernel(value, kappa, swap, near, far):
    levels, rows, _ = value.shape
    lev = lax.axis_index("lev")

    def row_of(is_kappa, e, r):
        if e >= levels:
            start = (e - levels + (STEPS if is_kappa else 0)) * rows
            return swap[start + r : start + r + 1, :]
        at = level_at(e, levels, lev)
        k = kappa[at, r : r + 1, :]
        return k if is_kappa else jnp.sqrt(k) * value[at, r : r + 1, :]

    pack_rows(row_plan(levels, True), row_of, near, far, rows)


def prepare_kernel(blocks, perturbations_h, innovation_h, mask_h, interp, huber, perturbations, innovation, mask, done):
    copies = copies_of((perturbations_h, innovation_h, mask_h), (perturbations, innovation, mask), done)
    for copy in copies:
        copy.start()
    width = interp.shape[1]
    coarse = interp.shape[0]
    refine = width // coarse
    shape = (coarse, width)
    column = iota(shape, 1)
    at = iota(shape, 0)
    cell = column // refine
    fraction = (column % refine).astype(F32) * (1.0 / refine)
    following = jnp.where(cell == coarse - 1, 0, cell + 1)
    below = cell == at
    interp[...] = (
        jnp.where(below, 1.0 - fraction, 0.0) + jnp.where(following == at, fraction, 0.0)
    ).astype(BF16)
    spread = jnp.where(below, 1.0, 0.0).astype(BF16)
    huber[...] = jnp.dot(blocks[...].astype(F32).astype(BF16), spread, preferred_element_type=F32)
    for copy in copies:
        copy.wait()


def pack_weighted_kernel(scaled, swap, near, far):
    levels, rows, _ = scaled.shape

    def row_of(is_kappa, e, r):
        if e >= levels:
            start = (e - levels) * rows
            return swap[start + r : start + r + 1, :]
        return scaled[e, r : r + 1, :]

    pack_rows(row_plan(levels, False), row_of, near, far, rows)


def unpack_rows(plan, state, kappa_ext, near, far, rows):
    def fill(low, high):
        is_first = lax.axis_index("wide") == 0
        for j, (is_kappa, d, e) in enumerate(plan):
            target = kappa_ext if is_kappa else state
            target[e, 2 * rows - d : 2 * rows - d + 1, :] = jnp.where(is_first, 0.0, low[j : j + 1, :])
            target[e, rows + d - 1 : rows + d, :] = high[j : j + 1, :]

    even = on_even()
    pl.when(even)(lambda: fill(far, near))
    pl.when(jnp.logical_not(even))(lambda: fill(near, far))


def diffuse_steps(state, kappa_ext, total, fold, edge, levels, rows, width, finish):
    is_last = lax.axis_index("wide") == lax.axis_size("wide") - 1
    tiles = width // LANES
    for step in range(STEPS):
        updated = levels + STEPS - 1 - step

        @pl.when(is_last)
        def _():
            for e in range(updated):
                edge[e : e + 1, :] = state[e, rows - 1 : rows, :]
            for t in range(tiles):
                index = jnp.broadcast_to(fold[:, t * LANES : (t + 1) * LANES], (8, LANES))
                lane = lax.rem(index, LANES)
                source = lax.div(index, LANES)
                found = jnp.zeros((8, LANES), F32)
                for q in range(tiles):
                    part = jnp.take_along_axis(
                        edge[:, q * LANES : (q + 1) * LANES], lane, axis=1, mode="promise_in_bounds"
                    )
                    found = jnp.where(source == q, part, found)
                for e in range(updated):
                    state[e, rows : rows + 1, t * LANES : (t + 1) * LANES] = found[e : e + 1, :]

        below = None
        for e in range(updated):
            whole = state[e]
            with_halo = step < STEPS - 1 and e < updated - 1
            kept = 2 * rows if with_halo else rows
            here = whole[:kept]
            above = state[e + 1, :kept, :]
            vertical = above if below is None else above + below[:kept]
            across = (
                pltpu.roll(whole, 2 * rows - 1, 0)[:kept]
                + pltpu.roll(whole, 1, 0)[:kept]
                + pltpu.roll(here, width - 1, 1)
                + pltpu.roll(here, 1, 1)
            )
            change = across + VERTICAL_WEIGHT * vertical - (4.0 + 2.0 * VERTICAL_WEIGHT) * here
            below = whole
            if step < STEPS - 1:
                state[e, :kept, :] = here + kappa_ext[e, :kept, :] * change
            if e < levels:
                if step == 0:
                    total[e] = change[:rows]
                elif step < STEPS - 1:
                    total[e] = total[e] + change[:rows]
                else:
                    finish(e, total[e] + change[:rows])


def static_kernel(value, kappa, swap, near, far, fold, diffused, kappa_ext, state, total, edge):
    levels, rows, width = value.shape
    lev = lax.axis_index("lev")
    zero = jnp.zeros((rows, width), F32)
    edge[...] = jnp.zeros(edge.shape, F32)
    for e in range(levels + STEPS):
        state[e, rows:, :] = zero
        if e < levels + STEPS - 1:
            kappa_ext[e, rows:, :] = zero
        if e < levels:
            at = level_at(e, levels, lev)
            k = kappa[at]
            kappa_ext[e, :rows, :] = k
            state[e, :rows, :] = jnp.sqrt(k) * value[at]
        else:
            start = (e - levels) * rows
            state[e, :rows, :] = swap[start : start + rows, :]
            if e < levels + STEPS - 1:
                start += STEPS * rows
                kappa_ext[e, :rows, :] = swap[start : start + rows, :]
    unpack_rows(row_plan(levels, True), state, kappa_ext, near, far, rows)

    def finish(e, change):
        at = level_at(e, levels, lev)
        diffused[at] = value[at] + jnp.sqrt(kappa[at]) * change

    diffuse_steps(state, kappa_ext, total, fold, edge, levels, rows, width, finish)


def weighted_kernel(
    value, weighted, kappa, kappa_ext, scaled, swap, near, far, fold, gradient_h, gradient, state, ring, total, edge, done
):
    levels, rows, width = value.shape
    lev = lax.axis_index("lev")
    zero = jnp.zeros((rows, width), F32)
    edge[...] = jnp.zeros(edge.shape, F32)
    for e in range(levels + STEPS):
        state[e, rows:, :] = zero
        if e < levels:
            state[e, :rows, :] = scaled[e]
        else:
            start = (e - levels) * rows
            state[e, :rows, :] = swap[start : start + rows, :]
    unpack_rows(row_plan(levels, False), state, ring, near, far, rows)

    def finish(e, change):
        at = level_at(e, levels, lev)
        gradient[e] = value[at] + (weighted[at] + jnp.sqrt(kappa[at]) * change)
        copy = pltpu.make_async_copy(gradient.at[e], gradient_h.at[at], done.at[e])
        copy.start()
        leaving.append(copy)

    leaving = []
    diffuse_steps(state, kappa_ext, total, fold, edge, levels, rows, width, finish)
    for copy in leaving:
        copy.wait()


def ensemble_kernel(
    windows, interp, perturbations, diffused, innovation, kappa, mask, huber, increment, weighted, scaled, swap, sent_h, sent, coarse, terms, done
):
    members, levels, rows, width = perturbations.shape
    lev = lax.axis_index("lev")
    coarse[...] = dot_split(windows[...], interp[...])
    fraction = iota((rows, width), 0).astype(F32) * (1.0 / rows)

    def add_group(first, sums):
        sums = list(sums)
        for m in range(min(GROUP, members)):
            at = first + m
            fine = (1.0 - fraction) * coarse[pl.ds(at, 1), :] + fraction * coarse[pl.ds(members + at, 1), :]
            for l in range(levels):
                sums[l] = sums[l] + fine * perturbations[at, l].astype(F32)
        return tuple(sums)

    sums = tuple(jnp.zeros((rows, width), F32) for _ in range(levels))
    if members <= GROUP:
        sums = add_group(0, sums)
    else:
        sums = lax.fori_loop(0, members // GROUP, lambda g, s: add_group(g * GROUP, s), sums)
    ocean = mask[...].astype(F32)
    scale = (members - 1) ** (-0.5)
    for l in range(levels):
        grown = ocean * (scale * sums[l] + diffused[l])
        increment[l] = grown
        misfit = grown - innovation[l]
        weight = jnp.where(
            huber[l : l + 1, :] > 0.5, HUBER_EDGE / jnp.maximum(jnp.abs(misfit), HUBER_EDGE), 1.0
        )
        weighted[l] = ocean * weight * misfit
    member_terms(perturbations, weighted, interp, sent, terms)
    leave = pltpu.make_async_copy(sent, sent_h, done.at[0])
    leave.start()
    for l in range(levels):
        rooted = jnp.sqrt(kappa[l]) * weighted[l]
        entry = level_at(l, levels, lev)
        scaled[entry] = rooted

        @pl.when(entry > 0)
        def _():
            swap[pl.ds(pl.multiple_of((levels - 1 - entry) * rows, 8), rows), :] = rooted

    leave.wait()


def member_terms(perturbations, weighted, interp, sent, terms):
    members, levels, rows, _ = perturbations.shape
    group = min(GROUP, members)
    scale = (members - 1) ** (-0.5)
    shape = (2 * group, group * rows)
    pair = iota(shape, 0)
    column = iota(shape, 1)
    fraction = (column % rows).astype(F32) * (1.0 / rows)
    share = jnp.where(pair % 2 == 0, 1.0 - fraction, fraction)
    share = jnp.where(column // rows == pair // 2, share, 0.0).astype(BF16)
    held = [weighted[l] for l in range(levels)]

    def one_group(first):
        for m in range(group):
            term = held[0] * perturbations[first + m, 0].astype(F32)
            for l in range(1, levels):
                term = term + held[l] * perturbations[first + m, l].astype(F32)
            terms[m * rows : (m + 1) * rows, :] = term
        narrow = dot_split(terms[...], interp[...], ((1,), (1,)))
        narrow = sum_parts(narrow, lambda part: dot(share, part))
        for target in range(2):
            start = pl.multiple_of(2 * (target * members + first), 8)
            sent[pl.ds(start, 2 * group), :] = scale * narrow

    if members <= GROUP:
        one_group(0)
    else:
        lax.fori_loop(0, members // GROUP, lambda g, c: (one_group(g * GROUP), c)[1], 0)


def member_kernel(received, member, rows_f, cols_f, gradient):
    coarse = rows_f.shape[0]
    main, following = [
        received[pl.ds(row, coarse, stride=2), :] + received[pl.ds(2 * coarse + row, coarse, stride=2), :] for row in range(2)
    ]
    at = iota(main.shape, 0)
    smooth = main + jnp.where(at == 0, 0.0, pltpu.roll(following, 1, 0))
    smooth = smooth + jnp.where(at == coarse - 1, following, 0.0)
    right_done = dot_precise(smooth, cols_f[...], ((1,), (1,)))
    gradient[0] = member[0] + dot_precise(rows_f[...], right_done, ((0,), (0,)))


def call(kernel, outs, scratch=(), results=()):
    names = [n for n in inspect.signature(kernel).parameters]
    count = len(names) - len(outs) - len(scratch)
    in_hbm = [n.endswith("_h") for n in names]

    def out_type(i, shape, dtype):
        if i in results:
            return jax.ShapeDtypeStruct(shape, dtype)
        return (pltpu.HBM if in_hbm[count + i] else pltpu.VMEM)(shape, dtype)

    def spec(hbm):
        return pl.BlockSpec(memory_space=pltpu.HBM if hbm else pltpu.VMEM)

    run = pl.pallas_call(
        kernel,
        in_specs=[spec(in_hbm[i]) for i in range(count)],
        out_specs=[spec(in_hbm[count + i]) for i in range(len(outs))],
        out_shape=[out_type(i, shape, dtype) for i, (shape, dtype) in enumerate(outs)],
        scratch_shapes=[
            pltpu.SemaphoreType.DMA(shape) if dtype is None else pltpu.VMEM(shape, dtype) for shape, dtype in scratch
        ],
        cost_estimate=pl.CostEstimate(flops=100000, transcendentals=0, bytes_accessed=0),
        compiler_params=pltpu.CompilerParams(vmem_limit_bytes=VMEM_BYTES),
    )

    def place(args):
        return [pltpu.with_memory_space_constraint(a, pltpu.HBM if in_hbm[i] else pltpu.VMEM) for i, a in enumerate(args)]

    return lambda *args: run(*place(args))


def on_device(
    member_control,
    static_control,
    perturbations,
    innovation,
    diffusivity,
    rows_factor,
    column_factor,
    ocean_mask,
    huber_blocks,
    fold_map,
):
    members, levels, rows, width = perturbations.shape
    wide, lev = lax.axis_size("wide"), lax.axis_size("lev")
    coarse_rows, coarse = rows_factor.shape[0], column_factor.shape[0]
    assert lev == 2 and members == wide and coarse_rows == wide and rows == 8 and levels >= STEPS
    assert wide % 2 == 0
    pairs = [(i, i ^ 1) for i in range(wide)]
    between = [(edge + l, edge + 1 - l) for edge in (0, 2 * wide - 2) for l in range(2)]
    for i in range(1, wide - 1, 2):
        for l in range(2):
            between += [(2 * i + l, 2 * i + 2 + l), (2 * i + 2 + l, 2 * i + l)]
    partner = [(0, 1), (1, 0)]
    cell = (levels, rows, width)

    swap, windows, value, kappa, member, rows_f, cols_f, blocks, fold = call(
        start_kernel,
        [
            (((2 * STEPS - 1) * rows, width), F32),
            ((2 * coarse_rows, coarse), F32),
            (cell, F32),
            (cell, F32),
            (member_control.shape, F32),
            (rows_factor.shape, F32),
            (column_factor.shape, F32),
            ((levels, coarse), jnp.int32),
            ((1, width), jnp.int32),
        ],
        [((2 * coarse_rows, coarse), F32), ((8,), None)],
    )(
        static_control,
        diffusivity,
        member_control,
        rows_factor,
        column_factor,
        huber_blocks.reshape(levels, coarse),
        fold_map.reshape(1, width),
    )
    swap = lax.ppermute(swap, "lev", partner)
    windows = lax.all_to_all(windows.reshape(2 * wide, 1, coarse), ("lev", "wide"), 0, 0, tiled=True)
    windows = windows.reshape(2 * members, coarse)
    count = padded_rows(levels, True)
    near, far = call(pack_static_kernel, [((count, width), F32), ((count, width), F32)])(value, kappa, swap)
    far = lax.ppermute(far, ("wide", "lev"), between)
    near = lax.ppermute(near, "wide", pairs)
    interp, huber, perturbations, innovation, mask = call(
        prepare_kernel,
        [
            ((coarse, width), BF16),
            ((levels, width), F32),
            (perturbations.shape, BF16),
            (cell, F32),
            (ocean_mask.shape, jnp.int32),
        ],
        [((3,), None)],
    )(blocks, perturbations, innovation, ocean_mask)
    entries = levels + STEPS
    diffused, kappa_ext = call(
        static_kernel,
        [(cell, F32), ((entries - 1, 2 * rows, width), F32)],
        [((entries, 2 * rows, width), F32), (cell, F32), ((8, width), F32)],
    )(value, kappa, swap, near, far, fold)
    increment, weighted, scaled, swap, sent = call(
        ensemble_kernel,
        [(cell, F32), (cell, F32), (cell, F32), ((STEPS * rows, width), F32), ((4 * members, coarse), F32)],
        [
            ((4 * members, coarse), F32),
            ((2 * members, width), F32),
            ((min(GROUP, members) * rows, width), F32),
            ((1,), None),
        ],
    )(windows, interp, perturbations, diffused, innovation, kappa, mask, huber)
    swap = lax.ppermute(swap, "lev", partner)
    received = lax.all_to_all(sent.reshape(2 * members, 2, coarse), ("lev", "wide"), 0, 0, tiled=True)
    received = received.reshape(4 * members, coarse)
    count = padded_rows(levels, False)
    near, far = call(pack_weighted_kernel, [((count, width), F32), ((count, width), F32)])(scaled, swap)
    far = lax.ppermute(far, ("wide", "lev"), between)
    near = lax.ppermute(near, "wide", pairs)
    (static_gradient,) = call(
        weighted_kernel,
        [(cell, F32)],
        [
            (cell, F32),
            ((entries, 2 * rows, width), F32),
            ((8, LANES), F32),
            (cell, F32),
            ((8, width), F32),
            ((levels,), None),
        ],
    )(value, weighted, kappa, kappa_ext, scaled, swap, near, far, fold)
    (member_gradient,) = call(member_kernel, [(member_control.shape, F32)], results=(0,))(
        received, member, rows_f, cols_f
    )
    return (increment, member_gradient, static_gradient)


def solution(mesh):
    return jax.shard_map(
        on_device,
        mesh=mesh,
        in_specs=(
            P("wide", None, None),
            P("lev", "wide", None),
            P(None, "lev", "wide", None),
            P("lev", "wide", None),
            P("lev", "wide", None),
            P(),
            P(),
            P("wide", None),
            P("lev", "wide", None),
            P(),
        ),
        out_specs=(P("lev", "wide", None), P("wide", None, None), P("lev", "wide", None)),
        check_vma=False,
    )
```

```python
import inspect

import jax
import jax.numpy as jnp
from jax import lax
from jax.experimental import pallas as pl
from jax.experimental.pallas import tpu as pltpu
from jax.sharding import PartitionSpec as P


STEPS = 3
HUBER_EDGE = 1.0
VERTICAL_WEIGHT = 0.5
LANES = 128
GROUP = 16
VMEM_BYTES = 32 * 2**20
F32 = jnp.float32
BF16 = jnp.bfloat16


def dot(left, right, dims=((1,), (0,))):
    return lax.dot_general(left, right, (dims, ((), ())), preferred_element_type=F32)


def parts_of(array):
    high = array.astype(BF16)
    return high, (array - high.astype(F32)).astype(BF16)


def dot_precise(left, right, dims=((1,), (0,))):
    (left_high, left_low), (right_high, right_low) = parts_of(left), parts_of(right)
    return (dot(left_high, right_low, dims) + dot(left_low, right_high, dims)) + dot(left_high, right_high, dims)


def sum_parts(array, product):
    high, low = parts_of(array)
    return product(low) + product(high)


def dot_split(left, right, dims=((1,), (0,))):
    return sum_parts(left, lambda part: dot(part, right, dims))


def iota(shape, dim):
    return lax.broadcasted_iota(jnp.int32, shape, dim)


def level_at(entry, levels, lev):
    return jnp.where(lev == 0, entry, levels - 1 - entry)


def row_plan(levels, with_kappa):
    plan = [(False, d, e) for d in range(1, STEPS + 1) for e in range(levels + STEPS - d)]
    if with_kappa:
        plan += [(True, d, e) for d in range(1, STEPS) for e in range(levels + STEPS - 1 - d)]
    return plan


def padded_rows(levels, with_kappa):
    return -(-len(row_plan(levels, with_kappa)) // 8) * 8


def copies_of(sources, targets, done):
    return [pltpu.make_async_copy(s, t, done.at[i]) for i, (s, t) in enumerate(zip(sources, targets))]


def start_kernel(
    value_h, kappa_h, member_h, rows_h, cols_h, swap, windows_h, value, kappa, member, rows_f, cols_f, windows, done
):
    levels, rows, _ = value.shape
    coarse = rows_f.shape[0]
    lev = lax.axis_index("lev")
    sources = (member_h, cols_h, rows_h, kappa_h, value_h)
    copies = copies_of(sources, (member, cols_f, rows_f, kappa, value), done)
    for copy in copies:
        copy.start()
    for copy in copies[:3]:
        copy.wait()
    smoothed = dot_precise(rows_f[...], dot_precise(member[0], cols_f[...]))
    following = jnp.where(iota(smoothed.shape, 0) == coarse - 1, smoothed, pltpu.roll(smoothed, coarse - 1, 0))
    mine = jnp.where(lev == 0, smoothed, following)
    for target in range(2):
        windows[target * coarse : (target + 1) * coarse, :] = mine
    leave = pltpu.make_async_copy(windows, windows_h, done.at[len(copies)])
    leave.start()
    for copy in copies[3:]:
        copy.wait()
    for j in range(STEPS):
        at = level_at(levels - 1 - j, levels, lev)
        k = kappa[at]
        swap[j * rows : (j + 1) * rows, :] = jnp.sqrt(k) * value[at]
        if j < STEPS - 1:
            swap[(STEPS + j) * rows : (STEPS + j + 1) * rows, :] = k
    leave.wait()


def on_even():
    return lax.rem(lax.axis_index("wide"), 2) == 0


def pack_rows(plan, row_of, near, far, rows):
    def fill(upper, lower):
        for j, (is_kappa, d, e) in enumerate(plan):
            upper[j : j + 1, :] = row_of(is_kappa, e, rows - d)
            lower[j : j + 1, :] = row_of(is_kappa, e, d - 1)

    for out in (near, far):
        for j in range(len(plan), out.shape[0]):
            out[j : j + 1, :] = jnp.zeros((1, out.shape[1]), F32)
    even = on_even()
    pl.when(even)(lambda: fill(near, far))
    pl.when(jnp.logical_not(even))(lambda: fill(far, near))


def pack_static_kernel(value, kappa, swap, near, far):
    levels, rows, _ = value.shape
    lev = lax.axis_index("lev")

    def row_of(is_kappa, e, r):
        if e >= levels:
            start = (e - levels + (STEPS if is_kappa else 0)) * rows
            return swap[start + r : start + r + 1, :]
        at = level_at(e, levels, lev)
        k = kappa[at, r : r + 1, :]
        return k if is_kappa else jnp.sqrt(k) * value[at, r : r + 1, :]

    pack_rows(row_plan(levels, True), row_of, near, far, rows)


def prepare_kernel(
    blocks_h, fold_h, perturbations_h, innovation_h, mask_h, interp, huber, fold, perturbations, innovation, mask, blocks, done
):
    copies = copies_of(
        (blocks_h, fold_h, perturbations_h, innovation_h, mask_h), (blocks, fold, perturbations, innovation, mask), done
    )
    for copy in copies:
        copy.start()
    width = interp.shape[1]
    coarse = interp.shape[0]
    refine = width // coarse
    shape = (coarse, width)
    column = iota(shape, 1)
    at = iota(shape, 0)
    cell = column // refine
    fraction = (column % refine).astype(F32) * (1.0 / refine)
    following = jnp.where(cell == coarse - 1, 0, cell + 1)
    below = cell == at
    interp[...] = (
        jnp.where(below, 1.0 - fraction, 0.0) + jnp.where(following == at, fraction, 0.0)
    ).astype(BF16)
    spread = jnp.where(below, 1.0, 0.0).astype(BF16)
    copies[0].wait()
    huber[...] = jnp.dot(blocks[...].astype(F32).astype(BF16), spread, preferred_element_type=F32)
    for copy in copies[1:]:
        copy.wait()


def pack_weighted_kernel(scaled, swap, near, far):
    levels, rows, _ = scaled.shape

    def row_of(is_kappa, e, r):
        if e >= levels:
            start = (e - levels) * rows
            return swap[start + r : start + r + 1, :]
        return scaled[e, r : r + 1, :]

    pack_rows(row_plan(levels, False), row_of, near, far, rows)


def unpack_rows(plan, state, kappa_ext, near, far, rows):
    def fill(low, high):
        is_first = lax.axis_index("wide") == 0
        for j, (is_kappa, d, e) in enumerate(plan):
            target = kappa_ext if is_kappa else state
            target[e, 2 * rows - d : 2 * rows - d + 1, :] = jnp.where(is_first, 0.0, low[j : j + 1, :])
            target[e, rows + d - 1 : rows + d, :] = high[j : j + 1, :]

    even = on_even()
    pl.when(even)(lambda: fill(far, near))
    pl.when(jnp.logical_not(even))(lambda: fill(near, far))


def diffuse_steps(state, kappa_ext, total, fold, edge, levels, rows, width, finish):
    is_last = lax.axis_index("wide") == lax.axis_size("wide") - 1
    tiles = width // LANES
    for step in range(STEPS):
        updated = levels + STEPS - 1 - step

        @pl.when(is_last)
        def _():
            for e in range(updated):
                edge[e : e + 1, :] = state[e, rows - 1 : rows, :]
            for t in range(tiles):
                index = jnp.broadcast_to(fold[:, t * LANES : (t + 1) * LANES], (8, LANES))
                lane = lax.rem(index, LANES)
                source = lax.div(index, LANES)
                found = jnp.zeros((8, LANES), F32)
                for q in range(tiles):
                    part = jnp.take_along_axis(
                        edge[:, q * LANES : (q + 1) * LANES], lane, axis=1, mode="promise_in_bounds"
                    )
                    found = jnp.where(source == q, part, found)
                for e in range(updated):
                    state[e, rows : rows + 1, t * LANES : (t + 1) * LANES] = found[e : e + 1, :]

        below = None
        for e in range(updated):
            whole = state[e]
            with_halo = step < STEPS - 1 and e < updated - 1
            kept = 2 * rows if with_halo else rows
            here = whole[:kept]
            above = state[e + 1, :kept, :]
            vertical = above if below is None else above + below[:kept]
            across = (
                pltpu.roll(whole, 2 * rows - 1, 0)[:kept]
                + pltpu.roll(whole, 1, 0)[:kept]
                + pltpu.roll(here, width - 1, 1)
                + pltpu.roll(here, 1, 1)
            )
            change = across + VERTICAL_WEIGHT * vertical - (4.0 + 2.0 * VERTICAL_WEIGHT) * here
            below = whole
            if step < STEPS - 1:
                state[e, :kept, :] = here + kappa_ext[e, :kept, :] * change
            if e < levels:
                if step == 0:
                    total[e] = change[:rows]
                elif step < STEPS - 1:
                    total[e] = total[e] + change[:rows]
                else:
                    finish(e, total[e] + change[:rows])


def static_kernel(value, kappa, swap, near, far, fold, diffused, kappa_ext, state, total, edge):
    levels, rows, width = value.shape
    lev = lax.axis_index("lev")
    zero = jnp.zeros((rows, width), F32)
    edge[...] = jnp.zeros(edge.shape, F32)
    for e in range(levels + STEPS):
        state[e, rows:, :] = zero
        if e < levels + STEPS - 1:
            kappa_ext[e, rows:, :] = zero
        if e < levels:
            at = level_at(e, levels, lev)
            k = kappa[at]
            kappa_ext[e, :rows, :] = k
            state[e, :rows, :] = jnp.sqrt(k) * value[at]
        else:
            start = (e - levels) * rows
            state[e, :rows, :] = swap[start : start + rows, :]
            if e < levels + STEPS - 1:
                start += STEPS * rows
                kappa_ext[e, :rows, :] = swap[start : start + rows, :]
    unpack_rows(row_plan(levels, True), state, kappa_ext, near, far, rows)

    def finish(e, change):
        at = level_at(e, levels, lev)
        diffused[at] = value[at] + jnp.sqrt(kappa[at]) * change

    diffuse_steps(state, kappa_ext, total, fold, edge, levels, rows, width, finish)


def weighted_kernel(
    value, weighted, kappa, kappa_ext, scaled, swap, near, far, fold, gradient_h, gradient, state, ring, total, edge, done
):
    levels, rows, width = value.shape
    lev = lax.axis_index("lev")
    zero = jnp.zeros((rows, width), F32)
    edge[...] = jnp.zeros(edge.shape, F32)
    for e in range(levels + STEPS):
        state[e, rows:, :] = zero
        if e < levels:
            state[e, :rows, :] = scaled[e]
        else:
            start = (e - levels) * rows
            state[e, :rows, :] = swap[start : start + rows, :]
    unpack_rows(row_plan(levels, False), state, ring, near, far, rows)

    def finish(e, change):
        at = level_at(e, levels, lev)
        gradient[e] = value[at] + (weighted[at] + jnp.sqrt(kappa[at]) * change)
        copy = pltpu.make_async_copy(gradient.at[e], gradient_h.at[at], done.at[e])
        copy.start()
        leaving.append(copy)

    leaving = []
    diffuse_steps(state, kappa_ext, total, fold, edge, levels, rows, width, finish)
    for copy in leaving:
        copy.wait()


def ensemble_kernel(
    windows, interp, perturbations, diffused, innovation, kappa, mask, huber, increment, weighted, scaled, swap, sent_h, sent, coarse, terms, done
):
    members, levels, rows, width = perturbations.shape
    lev = lax.axis_index("lev")
    coarse[...] = dot_split(windows[...], interp[...])
    fraction = iota((rows, width), 0).astype(F32) * (1.0 / rows)

    def add_group(first, sums):
        sums = list(sums)
        for m in range(min(GROUP, members)):
            at = first + m
            fine = (1.0 - fraction) * coarse[pl.ds(at, 1), :] + fraction * coarse[pl.ds(members + at, 1), :]
            for l in range(levels):
                sums[l] = sums[l] + fine * perturbations[at, l].astype(F32)
        return tuple(sums)

    sums = tuple(jnp.zeros((rows, width), F32) for _ in range(levels))
    if members <= GROUP:
        sums = add_group(0, sums)
    else:
        sums = lax.fori_loop(0, members // GROUP, lambda g, s: add_group(g * GROUP, s), sums)
    ocean = mask[...].astype(F32)
    scale = (members - 1) ** (-0.5)
    for l in range(levels):
        grown = ocean * (scale * sums[l] + diffused[l])
        increment[l] = grown
        misfit = grown - innovation[l]
        weight = jnp.where(
            huber[l : l + 1, :] > 0.5, HUBER_EDGE / jnp.maximum(jnp.abs(misfit), HUBER_EDGE), 1.0
        )
        weighted[l] = ocean * weight * misfit
    member_terms(perturbations, weighted, interp, sent, terms)
    leave = pltpu.make_async_copy(sent, sent_h, done.at[0])
    leave.start()
    for l in range(levels):
        rooted = jnp.sqrt(kappa[l]) * weighted[l]
        entry = level_at(l, levels, lev)
        scaled[entry] = rooted

        @pl.when(entry > 0)
        def _():
            swap[pl.ds(pl.multiple_of((levels - 1 - entry) * rows, 8), rows), :] = rooted

    leave.wait()


def member_terms(perturbations, weighted, interp, sent, terms):
    members, levels, rows, _ = perturbations.shape
    group = min(GROUP, members)
    scale = (members - 1) ** (-0.5)
    shape = (2 * group, group * rows)
    pair = iota(shape, 0)
    column = iota(shape, 1)
    fraction = (column % rows).astype(F32) * (1.0 / rows)
    share = jnp.where(pair % 2 == 0, 1.0 - fraction, fraction)
    share = jnp.where(column // rows == pair // 2, share, 0.0).astype(BF16)
    held = [weighted[l] for l in range(levels)]

    def one_group(first):
        for m in range(group):
            term = held[0] * perturbations[first + m, 0].astype(F32)
            for l in range(1, levels):
                term = term + held[l] * perturbations[first + m, l].astype(F32)
            terms[m * rows : (m + 1) * rows, :] = term
        narrow = dot_split(terms[...], interp[...], ((1,), (1,)))
        narrow = sum_parts(narrow, lambda part: dot(share, part))
        for target in range(2):
            start = pl.multiple_of(2 * (target * members + first), 8)
            sent[pl.ds(start, 2 * group), :] = scale * narrow

    if members <= GROUP:
        one_group(0)
    else:
        lax.fori_loop(0, members // GROUP, lambda g, c: (one_group(g * GROUP), c)[1], 0)


def member_kernel(received, member, rows_f, cols_f, gradient):
    coarse = rows_f.shape[0]
    main, following = [
        received[pl.ds(row, coarse, stride=2), :] + received[pl.ds(2 * coarse + row, coarse, stride=2), :] for row in range(2)
    ]
    at = iota(main.shape, 0)
    smooth = main + jnp.where(at == 0, 0.0, pltpu.roll(following, 1, 0))
    smooth = smooth + jnp.where(at == coarse - 1, following, 0.0)
    right_done = dot_precise(smooth, cols_f[...], ((1,), (1,)))
    gradient[0] = member[0] + dot_precise(rows_f[...], right_done, ((0,), (0,)))


def call(kernel, outs, scratch=(), results=()):
    names = [n for n in inspect.signature(kernel).parameters]
    count = len(names) - len(outs) - len(scratch)
    in_hbm = [n.endswith("_h") for n in names]

    def out_type(i, shape, dtype):
        if i in results:
            return jax.ShapeDtypeStruct(shape, dtype)
        return (pltpu.HBM if in_hbm[count + i] else pltpu.VMEM)(shape, dtype)

    def spec(hbm):
        return pl.BlockSpec(memory_space=pltpu.HBM if hbm else pltpu.VMEM)

    run = pl.pallas_call(
        kernel,
        in_specs=[spec(in_hbm[i]) for i in range(count)],
        out_specs=[spec(in_hbm[count + i]) for i in range(len(outs))],
        out_shape=[out_type(i, shape, dtype) for i, (shape, dtype) in enumerate(outs)],
        scratch_shapes=[
            pltpu.SemaphoreType.DMA(shape) if dtype is None else pltpu.VMEM(shape, dtype) for shape, dtype in scratch
        ],
        cost_estimate=pl.CostEstimate(flops=100000, transcendentals=0, bytes_accessed=0),
        compiler_params=pltpu.CompilerParams(vmem_limit_bytes=VMEM_BYTES),
    )

    def place(args):
        return [pltpu.with_memory_space_constraint(a, pltpu.HBM if in_hbm[i] else pltpu.VMEM) for i, a in enumerate(args)]

    return lambda *args: run(*place(args))


def on_device(
    member_control,
    static_control,
    perturbations,
    innovation,
    diffusivity,
    rows_factor,
    column_factor,
    ocean_mask,
    huber_blocks,
    fold_map,
):
    members, levels, rows, width = perturbations.shape
    wide, lev = lax.axis_size("wide"), lax.axis_size("lev")
    coarse_rows, coarse = rows_factor.shape[0], column_factor.shape[0]
    assert lev == 2 and members == wide and coarse_rows == wide and rows == 8 and levels >= STEPS
    assert wide % 2 == 0
    pairs = [(i, i ^ 1) for i in range(wide)]
    between = [(edge + l, edge + 1 - l) for edge in (0, 2 * wide - 2) for l in range(2)]
    for i in range(1, wide - 1, 2):
        for l in range(2):
            between += [(2 * i + l, 2 * i + 2 + l), (2 * i + 2 + l, 2 * i + l)]
    partner = [(0, 1), (1, 0)]
    cell = (levels, rows, width)

    swap, windows, value, kappa, member, rows_f, cols_f = call(
        start_kernel,
        [
            (((2 * STEPS - 1) * rows, width), F32),
            ((2 * coarse_rows, coarse), F32),
            (cell, F32),
            (cell, F32),
            (member_control.shape, F32),
            (rows_factor.shape, F32),
            (column_factor.shape, F32),
        ],
        [((2 * coarse_rows, coarse), F32), ((8,), None)],
    )(
        static_control,
        diffusivity,
        member_control,
        rows_factor,
        column_factor,
    )
    swap = lax.ppermute(swap, "lev", partner)
    windows = lax.all_to_all(windows.reshape(2 * wide, 1, coarse), ("lev", "wide"), 0, 0, tiled=True)
    windows = windows.reshape(2 * members, coarse)
    count = padded_rows(levels, True)
    near, far = call(pack_static_kernel, [((count, width), F32), ((count, width), F32)])(value, kappa, swap)
    far = lax.ppermute(far, ("wide", "lev"), between)
    near = lax.ppermute(near, "wide", pairs)
    interp, huber, fold, perturbations, innovation, mask = call(
        prepare_kernel,
        [
            ((coarse, width), BF16),
            ((levels, width), F32),
            ((1, width), jnp.int32),
            (perturbations.shape, BF16),
            (cell, F32),
            (ocean_mask.shape, jnp.int32),
        ],
        [((levels, coarse), jnp.int32), ((5,), None)],
    )(huber_blocks.reshape(levels, coarse), fold_map.reshape(1, width), perturbations, innovation, ocean_mask)
    entries = levels + STEPS
    diffused, kappa_ext = call(
        static_kernel,
        [(cell, F32), ((entries - 1, 2 * rows, width), F32)],
        [((entries, 2 * rows, width), F32), (cell, F32), ((8, width), F32)],
    )(value, kappa, swap, near, far, fold)
    increment, weighted, scaled, swap, sent = call(
        ensemble_kernel,
        [(cell, F32), (cell, F32), (cell, F32), ((STEPS * rows, width), F32), ((4 * members, coarse), F32)],
        [
            ((4 * members, coarse), F32),
            ((2 * members, width), F32),
            ((min(GROUP, members) * rows, width), F32),
            ((1,), None),
        ],
    )(windows, interp, perturbations, diffused, innovation, kappa, mask, huber)
    swap = lax.ppermute(swap, "lev", partner)
    received = lax.all_to_all(sent.reshape(2 * members, 2, coarse), ("lev", "wide"), 0, 0, tiled=True)
    received = received.reshape(4 * members, coarse)
    count = padded_rows(levels, False)
    near, far = call(pack_weighted_kernel, [((count, width), F32), ((count, width), F32)])(scaled, swap)
    far = lax.ppermute(far, ("wide", "lev"), between)
    near = lax.ppermute(near, "wide", pairs)
    (static_gradient,) = call(
        weighted_kernel,
        [(cell, F32)],
        [
            (cell, F32),
            ((entries, 2 * rows, width), F32),
            ((8, LANES), F32),
            (cell, F32),
            ((8, width), F32),
            ((levels,), None),
        ],
    )(value, weighted, kappa, kappa_ext, scaled, swap, near, far, fold)
    (member_gradient,) = call(member_kernel, [(member_control.shape, F32)], results=(0,))(
        received, member, rows_f, cols_f
    )
    return (increment, member_gradient, static_gradient)


def solution(mesh):
    return jax.shard_map(
        on_device,
        mesh=mesh,
        in_specs=(
            P("wide", None, None),
            P("lev", "wide", None),
            P(None, "lev", "wide", None),
            P("lev", "wide", None),
            P("lev", "wide", None),
            P(),
            P(),
            P("wide", None),
            P("lev", "wide", None),
            P(),
        ),
        out_specs=(P("lev", "wide", None), P("wide", None, None), P("lev", "wide", None)),
        check_vma=False,
    )
```
